128 devices in a mesh: clus: 32 (over x, y, core), lab: 4 (over z).
Axes of the slice: x: 4, y: 4, z: 4, core: 2. Of those that a mesh axis runs over, the one named last changes fastest.
Arguments:
- queries: bfloat16 [16384, 768], P(('clus', 'lab')), may hold values from -6 to 6
- visits: int32 [16384, 4], P(('clus', 'lab')), may hold values from 0 to 63, all different within a row; in each aligned block of 128 rows (0 to 127, 128 to 255, ...) at most 16 rows name the same one
- positives: int32 [16384, 4], P(('clus', 'lab')), may hold values from 0 to 4095
- weights: bfloat16 [64, 4096, 768], P('clus', 'lab'), may hold values from -0.21875 to 0.21875
- momentum: float32 [64, 4096, 768], P('clus', 'lab'), may hold values from -24 to 24
Outputs:
- query_grad: float32 [16384, 768], P(('clus', 'lab'))
- weights_new: bfloat16 [64, 4096, 768], P('clus', 'lab')
- momentum_new: float32 [64, 4096, 768], P('clus', 'lab')
The draws below stay inside these ranges and needn't reach their ends.
Inputs may be any that keep to these rules, and one draw needn't show every extreme that they name: `visits`: each query names 4 different clusters; among the 128 queries of one device at most 16 visit any one cluster.
All inputs are finite; a program needn't handle non-finite values.
Results may differ from the reference program's by a relative error of at most 0.006.
Values may be sent and summed in bfloat16 or wider, within the bound.
No kernel may reach another device: no remote copies, remote signals or barrier semaphores. Data moves between devices by JAX's collectives and lax.ppermute only.
A program may use at most 128 MiB of HBM per device.

```python
import math
import jax
import jax.numpy as jnp
import numpy as np
from jax import lax

D = 768
VISITS = 4
Q_DEV = 128
NCLUS = 64
CSIZE = 4096
CAP = 16
QUERIES = 16384


def plant(array, key, least, top_value):
    longest = array.shape.index(max(array.shape))
    spots = []
    for shift in (0, 1):
        where = [jax.random.randint(jax.random.fold_in(key, axis), (), 0, length) for axis, length in enumerate(array.shape)]
        where[longest] = (where[longest] + shift) % array.shape[longest]
        spots.append(tuple(where))
    return array.at[spots[0]].set(least).at[spots[1]].set(top_value)


def level_of(stream_key, shape, cuts, smallest, largest):
    factor_of = 1.0
    for axis_at, shards_of in cuts:
        heights = jax.random.uniform(jax.random.fold_in(jax.random.fold_in(stream_key, 6), axis_at), (shards_of,), jnp.float32, smallest / len(cuts), largest / len(cuts))
        factor_of = factor_of * jnp.repeat(jnp.exp(heights), shape[axis_at] // shards_of).reshape((-1,) + (1,) * (len(shape) - 1 - axis_at))
    return factor_of


def deal_out(stream_key, own, number, rows, count, top, reach, skew):
    sequence = jax.random.permutation(stream_key, count)
    packed, ordinary = portions_of(count, rows * top, reach, skew, True), portions_of(count, rows * top, reach, skew, False)
    places = jnp.arange(count)

    def named(tallies, turn):
        used = int((tallies > 0).sum())
        fixed = max(1, used // 4)
        passed = fixed + (places - fixed + turn * (used - fixed)) % max(1, count - fixed)
        return jnp.zeros((count,), jnp.int32).at[sequence[jnp.where(places < fixed, places, passed)]].set(jnp.asarray(tallies, jnp.int32))

    tallies = jnp.where(number % 4 == 0, named(packed, number // 4), named(ordinary, number - number // 4 - 1))
    mixed = jax.random.permutation(jax.random.fold_in(own, 3), count)
    donor, taker = mixed[0:count // 2 * 2:2], mixed[1:count // 2 * 2:2]
    room = jnp.minimum(tallies[donor] - 1, reach - tallies[taker]) // 2
    room = jnp.where((donor == sequence[0]) | (taker == sequence[0]) | (tallies[taker] == 0), 0, jnp.maximum(room, 0))
    passed = jax.random.randint(jax.random.fold_in(own, 4), (count // 2,), 0, 1 << 20) % (room + 1)
    tallies = tallies.at[donor].add(-passed).at[taker].add(passed)
    labels = jnp.searchsorted(jnp.cumsum(tallies), jnp.arange(rows * top), side="right").astype(jnp.int32)
    listing = labels.reshape(top, rows).T
    listing = listing[jax.random.permutation(jax.random.fold_in(own, 1), rows)]
    turn = jax.random.randint(jax.random.fold_in(own, 2), (rows, 1), 0, top)
    return jnp.take_along_axis(listing, (jnp.arange(top)[None, :] + turn) % top, axis=1)


def portions_of(count, total, most, skew, full):
    weights = [(1 << 20) // math.isqrt(rank ** skew) + 1 for rank in range(1, count + 1)]
    largest = most if full else min(most, max(-(-total // count), total * weights[0] // sum(weights)))
    least = 1 if total - largest >= count - 1 else 0
    given, spare = [largest] + [least] * (count - 1), total - largest - least * (count - 1)
    while spare > 0:
        movable = [i for i in range(1, count) if given[i] < largest] or [i for i in range(1, count) if given[i] < most]
        pool, left = sum([weights[i] for i in movable]), spare
        for i in movable:
            extra = min(most - given[i], max(1, left * weights[i] // pool), spare)
            given[i] = given[i] + extra
            spare = spare - extra
    return np.array(given)


def bell_draw(rng, shape, width, bound, pieces=(), held_as=jnp.bfloat16):
    level = level_of(rng, shape, pieces, -0.22, 0.18) if pieces else 1.0
    result = jax.random.normal(rng, shape, jnp.float32) * width * level
    return jnp.minimum(jnp.maximum(result, -bound), bound).astype(held_as)


def setup_inputs(seed: int = 0) -> dict:
    arg_keys = jax.random.split(jax.random.key(seed), 6)
    queries = bell_draw(arg_keys[0], (QUERIES, D), 1.0, 6.0, ((0, 128),))
    visits_keys = jax.random.split(jax.random.fold_in(arg_keys[1], 1), QUERIES // Q_DEV)
    visits_turns = jax.random.permutation(jax.random.fold_in(arg_keys[1], 3), QUERIES // Q_DEV)
    visits = jax.vmap(lambda own, number: deal_out(jax.random.fold_in(arg_keys[1], 2), own, number, Q_DEV, NCLUS, VISITS, CAP, 2))(visits_keys, visits_turns).reshape((QUERIES, VISITS))
    positives = plant(jax.random.randint(arg_keys[2], (QUERIES, VISITS), 0, CSIZE), jax.random.fold_in(arg_keys[2], 1), 0, CSIZE - 1).astype(jnp.int32)
    weights = bell_draw(arg_keys[3], (NCLUS, CSIZE, D), D ** -0.5, 0.21875, ((0, 32), (1, 4)))
    momentum = bell_draw(arg_keys[4], (NCLUS, CSIZE, D), 4.0, 24.0, ((0, 32), (1, 4)), jnp.float32)
    return {"queries": queries, "visits": visits, "positives": positives, "weights": weights, "momentum": momentum}


momentum_decay = 0.9
step_rate = 0.002


def reference(queries, visits, positives, weights, momentum):
    ndevices = QUERIES // Q_DEV
    flat_visits = visits.reshape(ndevices, Q_DEV * VISITS)
    one_hot = (flat_visits[:, :, None] == jnp.arange(NCLUS, dtype=jnp.int32)[None, None, :]).astype(jnp.int32)
    before = jnp.cumsum(one_hot, axis=1) - one_hot
    ranks = jnp.sum(before * one_hot, axis=2)
    columns = jnp.arange(ndevices, dtype=jnp.int32)[:, None] * CAP + ranks
    visit_ids = jnp.arange(QUERIES * VISITS, dtype=jnp.int32).reshape(ndevices, Q_DEV * VISITS)
    table = jnp.full((NCLUS, ndevices * CAP), -1, jnp.int32)
    table = table.at[flat_visits.reshape(-1), columns.reshape(-1)].set(visit_ids.reshape(-1))
    flat_positives = positives.reshape(-1)
    label_ids = jnp.arange(CSIZE, dtype=jnp.int32)

    def per_cluster(carry, inputs):
        ids, cluster_weights = inputs
        live = ids >= 0
        safe_ids = jnp.where(live, ids, 0)
        query_ids = (safe_ids // VISITS).astype(jnp.int32)
        arrived = queries[query_ids].astype(jnp.float32)
        label_tag = flat_positives[safe_ids]
        labels32 = cluster_weights.astype(jnp.float32)
        logits = jnp.dot(arrived, labels32.T, precision=lax.Precision.HIGHEST)
        target = (label_tag[:, None] == label_ids[None, :]).astype(jnp.float32)
        grad = jnp.where(live[:, None], jax.nn.sigmoid(logits) - target, 0.0)
        grad_low = lax.optimization_barrier(grad.astype(jnp.bfloat16))
        grad32 = grad_low.astype(jnp.float32)
        query_part = jnp.dot(grad32, labels32, precision=lax.Precision.HIGHEST)
        carry = carry.at[query_ids].add(jnp.where(live[:, None], query_part, 0.0))
        label_grad = jnp.dot(grad32.T, arrived, precision=lax.Precision.HIGHEST)
        return carry, label_grad

    start = jnp.zeros((QUERIES, D), jnp.float32)
    query_grad, label_grad = lax.scan(per_cluster, start, (table, weights))
    momentum_new = momentum_decay * momentum + label_grad
    weights_new = (weights.astype(jnp.float32) - step_rate * momentum_new).astype(jnp.bfloat16)
    return (query_grad, weights_new, momentum_new)
```

```python
import jax
import jax.numpy as jnp
from jax import lax
from jax.experimental import pallas as pl
from jax.experimental.pallas import tpu as pltpu
from jax.sharding import PartitionSpec as P

momentum_decay = 0.9
step_rate = 0.002

CLUS = 32
LAB = 4
CAP = 16
NQ = 128
VISITS = 4
D = 768
EXTRA = 8
TAGS = 128
LABELS = 1024
BAND = 256
ROWS = CLUS * CAP


def ring(shift):
    return [(i, (i + shift) % LAB) for i in range(LAB)]


def picks(visits_t, parity):
    dest = lax.broadcasted_iota(jnp.int32, (CLUS, NQ), 0) * 2 + parity
    hit = visits_t[0:1, :] == dest
    for k in range(1, VISITS):
        hit = hit | (visits_t[k : k + 1, :] == dest)
    before = lax.broadcasted_iota(jnp.int32, (NQ, NQ), 0) < lax.broadcasted_iota(
        jnp.int32, (NQ, NQ), 1
    )
    rank = jnp.dot(
        hit.astype(jnp.float32).astype(jnp.bfloat16),
        before.astype(jnp.float32).astype(jnp.bfloat16),
        preferred_element_type=jnp.float32,
    )
    place = jnp.where(hit, rank, -1.0).astype(jnp.int32)
    slot = lax.broadcasted_iota(jnp.int32, (CLUS, CAP, NQ), 1)
    return (place[:, None, :] == slot).reshape(ROWS, NQ)


def as_bf16(flags):
    return flags.astype(jnp.float32).astype(jnp.bfloat16)


def labels_of(visits_t, positives_t, parity):
    dest = lax.broadcasted_iota(jnp.int32, (CLUS, NQ), 0) * 2 + parity
    label = jnp.zeros((CLUS, NQ), jnp.int32)
    for k in range(VISITS):
        label = label + jnp.where(visits_t[k : k + 1, :] == dest, positives_t[k : k + 1, :] + 1, 0)
    return label


def slot_labels(chosen, label):
    wide = jnp.broadcast_to(label[:, None, :], (CLUS, CAP, NQ)).reshape(ROWS, NQ)
    return jnp.sum(jnp.where(chosen, wide, 0), axis=1, keepdims=True) - 1


def own_kernel(visits_ref, positives_ref, queries_ref, box_ref, raw_ref):
    bf = jnp.bfloat16
    visits_t, positives_t = visits_ref[...], positives_ref[...]
    lane = lax.broadcasted_iota(jnp.int32, (ROWS, TAGS), 1)
    notes = jnp.zeros((ROWS, TAGS), jnp.float32)
    for parity in range(2):
        chosen = picks(visits_t, parity)
        label = slot_labels(chosen, labels_of(visits_t, positives_t, parity))
        high = label >> 6
        low = label & 63
        notes = jnp.where(lane == 2 * parity, high.astype(jnp.float32), notes)
        notes = jnp.where(lane == 2 * parity + 1, low.astype(jnp.float32), notes)
        if parity == 0:
            filled = jnp.dot(as_bf16(chosen), queries_ref[...], preferred_element_type=jnp.float32)
            box_ref[:, :D] = filled.astype(bf)
    box_ref[:, D:] = notes.astype(bf)
    raw_ref[:NQ] = queries_ref[...]
    values = visits_t.astype(jnp.float32)
    parts = [values[k : k + 1, :] for k in range(VISITS)]
    row = jnp.concatenate(parts + [jnp.zeros((1, D - VISITS * NQ), jnp.float32)], axis=1)
    raw_ref[NQ:] = jnp.concatenate([row, jnp.zeros((EXTRA - 1, D), jnp.float32)], axis=0).astype(bf)


def all_kernel(order_ref, raw_ref, box_ref):
    for k in range(LAB):
        s = order_ref[k]
        extra = raw_ref[s, NQ:].astype(jnp.float32)
        parts = [extra[0:1, j * NQ : (j + 1) * NQ] for j in range(VISITS)]
        visits_t = jnp.concatenate(parts, axis=0).astype(jnp.int32)
        filled = jnp.dot(
            as_bf16(picks(visits_t, 1)), raw_ref[s, :NQ], preferred_element_type=jnp.float32
        )
        box_ref[:, k] = filled.astype(jnp.bfloat16).reshape(CLUS, CAP, D)


def home_kernel(visits_ref, first_ref, second_ref, out_ref):
    total = jnp.zeros((NQ, D), jnp.float32)
    for parity, ref in ((0, first_ref), (1, second_ref)):
        chosen = as_bf16(picks(visits_ref[...], parity))
        total = total + lax.dot_general(
            chosen, ref[...], (((0,), (0,)), ((), ())), preferred_element_type=jnp.float32
        )
    out_ref[...] = total


def update_kernel(ga_ref, gb_ref, ra_ref, rb_ref, w_ref, m_ref, wo_ref, mo_ref):
    def apply(grad_ref, rows_ref):
        label_grad = lax.dot_general(
            grad_ref[...], rows_ref[...], (((0,), (0,)), ((), ())), preferred_element_type=jnp.float32
        )
        fresh = momentum_decay * m_ref[0] + label_grad
        mo_ref[0] = fresh
        wo_ref[0] = (w_ref[0].astype(jnp.float32) - step_rate * fresh).astype(jnp.bfloat16)

    @pl.when(pl.program_id(0) == 0)
    def _():
        apply(ga_ref, ra_ref)

    @pl.when(pl.program_id(0) == 1)
    def _():
        apply(gb_ref, rb_ref)


def update(grad_a, grad_b, rows_a, rows_b, weights, momentum):
    bands = LABELS // BAND
    n = LAB * ROWS
    whole = pl.BlockSpec((n, D), lambda c, b: (0, 0))
    band = pl.BlockSpec((1, BAND, D), lambda c, b: (c, b, 0))
    return pl.pallas_call(
        update_kernel,
        grid=(2, bands),
        in_specs=[
            pl.BlockSpec((n, BAND), lambda c, b: (0, b * (1 - c) + (bands - 1) * c)),
            pl.BlockSpec((n, BAND), lambda c, b: (0, b * c)),
            whole,
            whole,
            band,
            band,
        ],
        out_specs=(band, band),
        out_shape=(
            jax.ShapeDtypeStruct(weights.shape, weights.dtype),
            jax.ShapeDtypeStruct(momentum.shape, momentum.dtype),
        ),
        compiler_params=pltpu.CompilerParams(
            dimension_semantics=("arbitrary", "arbitrary"), vmem_limit_bytes=40 << 20
        ),
        cost_estimate=pl.CostEstimate(
            flops=2 * 2 * n * LABELS * D, bytes_accessed=36 << 20, transcendentals=0
        ),
        name="update",
    )(grad_a, grad_b, rows_a, rows_b, weights, momentum)


def grads(rows, tag, weights, offsets):
    logits = jnp.einsum("rd,bd->rb", rows, weights, preferred_element_type=jnp.float32)
    target = (tag == offsets[None, :]).astype(jnp.float32)
    grad = (jax.nn.sigmoid(logits) - target).astype(jnp.bfloat16)
    part = jnp.einsum("rb,bd->rd", grad, weights, preferred_element_type=jnp.float32)
    return grad, part.astype(jnp.bfloat16)


def swap(x):
    return lax.all_to_all(x, "clus", split_axis=0, concat_axis=0, tiled=True)


def add(*terms):
    total = terms[0].astype(jnp.float32)
    for term in terms[1:]:
        total = total + term.astype(jnp.float32)
    return total.astype(jnp.bfloat16)


def scatter_sum(own, low, high, far):
    half = own.shape[0] // 2
    up = lax.ppermute(far[:half], "lab", ring(1))
    down = lax.ppermute(far[half:], "lab", ring(-1))
    up = jnp.concatenate([add(high[:half], up), high[half:]])
    down = jnp.concatenate([low[:half], add(low[half:], down)])
    up = lax.ppermute(up, "lab", ring(1))
    down = lax.ppermute(down, "lab", ring(-1))
    return add(own, up, down)


def shards(queries, visits, positives, weights, momentum):
    vt, pt = visits.T, positives.T
    bf = jnp.bfloat16
    me = lax.axis_index("lab")
    order = (me + jnp.array([0, 3, 1, 2], jnp.int32)) & 3

    box_a, raw = pl.pallas_call(
        own_kernel,
        out_shape=(
            jax.ShapeDtypeStruct((ROWS, D + TAGS), bf),
            jax.ShapeDtypeStruct((NQ + EXTRA, D), bf),
        ),
        name="own_box",
    )(vt, pt, queries)
    got_a = swap(box_a.reshape(CLUS, CAP, D + TAGS)).reshape(ROWS, D + TAGS)
    peers = lax.all_gather(raw, "lab", axis=0, tiled=False)
    box_b = pl.pallas_call(
        all_kernel,
        in_specs=[pl.BlockSpec(memory_space=pltpu.SMEM), pl.BlockSpec(memory_space=pltpu.VMEM)],
        out_shape=jax.ShapeDtypeStruct((CLUS, LAB, CAP, D), bf),
        name="all_box",
    )(order, peers)
    got_a, box_b = lax.optimization_barrier((got_a, box_b))
    got_b = swap(box_b.reshape(CLUS, LAB * CAP, D)).reshape(LAB * ROWS, D)

    half = ROWS // 2
    from_low = lax.ppermute(got_a, "lab", ring(1))
    from_high = lax.ppermute(got_a, "lab", ring(-1))
    far_low = lax.ppermute(from_low[:half], "lab", ring(1))
    far_high = lax.ppermute(from_high[half:], "lab", ring(-1))
    pieces = (got_a, from_low, from_high, far_low, far_high)
    rows_a = jnp.concatenate([p[:, :D] for p in pieces])
    notes = jnp.concatenate([p[:, D : D + 4] for p in pieces]).astype(jnp.int32)
    tag_a = notes[:, 0:1] * 64 + notes[:, 1:2]
    tag_b = notes[:, 2:3] * 64 + notes[:, 3:4]
    tag_b = jnp.moveaxis(tag_b.reshape(LAB, CLUS, CAP), 0, 1).reshape(LAB * ROWS, 1)

    offsets = me * LABELS + jnp.arange(LABELS, dtype=jnp.int32)
    grad_a, part_a = grads(rows_a, tag_a, weights[0], offsets)
    part_a = part_a.reshape(LAB, ROWS, D)
    home_a = scatter_sum(part_a[0], part_a[1], part_a[2], part_a[3])
    grad_b, part_b = grads(got_b, tag_b, weights[1], offsets)
    part_b = part_b.reshape(CLUS, LAB, CAP, D)
    home_b = scatter_sum(*[part_b[:, k].reshape(ROWS, D) for k in range(LAB)])
    home_a = swap(home_a.reshape(CLUS, CAP, D)).reshape(ROWS, D)
    home_b = swap(home_b.reshape(CLUS, CAP, D)).reshape(ROWS, D)
    weights_new, momentum_new = update(grad_a, grad_b, rows_a, got_b, weights, momentum)
    query_grad = pl.pallas_call(
        home_kernel, out_shape=jax.ShapeDtypeStruct((NQ, D), jnp.float32), name="home_sum"
    )(vt, home_a, home_b)
    return (query_grad, weights_new, momentum_new)


def solution(mesh):
    in_specs = (
        P(("clus", "lab"), None),
        P(("clus", "lab"), None),
        P(("clus", "lab"), None),
        P("clus", "lab", None),
        P("clus", "lab", None),
    )
    out_specs = (P(("clus", "lab"), None), P("clus", "lab", None), P("clus", "lab", None))
    return jax.shard_map(shards, mesh=mesh, in_specs=in_specs, out_specs=out_specs, check_vma=False)
```

```python
import jax
import jax.numpy as jnp
from jax import lax
from jax.experimental import pallas as pl
from jax.experimental.pallas import tpu as pltpu
from jax.sharding import PartitionSpec as P

momentum_decay = 0.9
step_rate = 0.002

CLUS = 32
LAB = 4
CAP = 16
NQ = 128
VISITS = 4
D = 768
EXTRA = 8
TAGS = 128
TILE = 256
SRC = TILE // (LAB * CAP)
STEPS = CLUS // SRC
LABELS = 1024
BAND = 256
ROWS = CLUS * CAP


def ring(shift):
    return [(i, (i + shift) % LAB) for i in range(LAB)]


def picks(visits_t, parity):
    dest = lax.broadcasted_iota(jnp.int32, (CLUS, NQ), 0) * 2 + parity
    hit = visits_t[0:1, :] == dest
    for k in range(1, VISITS):
        hit = hit | (visits_t[k : k + 1, :] == dest)
    before = lax.broadcasted_iota(jnp.int32, (NQ, NQ), 0) < lax.broadcasted_iota(
        jnp.int32, (NQ, NQ), 1
    )
    rank = jnp.dot(
        hit.astype(jnp.float32).astype(jnp.bfloat16),
        before.astype(jnp.float32).astype(jnp.bfloat16),
        preferred_element_type=jnp.float32,
    )
    place = jnp.where(hit, rank, -1.0).astype(jnp.int32)
    slot = lax.broadcasted_iota(jnp.int32, (CLUS, CAP, NQ), 1)
    return (place[:, None, :] == slot).reshape(ROWS, NQ)


def as_bf16(flags):
    return flags.astype(jnp.float32).astype(jnp.bfloat16)


def labels_of(visits_t, positives_t, parity):
    dest = lax.broadcasted_iota(jnp.int32, (CLUS, NQ), 0) * 2 + parity
    label = jnp.zeros((CLUS, NQ), jnp.int32)
    for k in range(VISITS):
        label = label + jnp.where(visits_t[k : k + 1, :] == dest, positives_t[k : k + 1, :] + 1, 0)
    return label


def slot_labels(chosen, label):
    wide = jnp.broadcast_to(label[:, None, :], (CLUS, CAP, NQ)).reshape(ROWS, NQ)
    return jnp.sum(jnp.where(chosen, wide, 0), axis=1, keepdims=True) - 1


def own_kernel(visits_ref, positives_ref, queries_ref, box_ref, raw_ref):
    bf = jnp.bfloat16
    visits_t, positives_t = visits_ref[...], positives_ref[...]
    lane = lax.broadcasted_iota(jnp.int32, (ROWS, TAGS), 1)
    notes = jnp.zeros((ROWS, TAGS), jnp.float32)
    for parity in range(2):
        chosen = picks(visits_t, parity)
        label = slot_labels(chosen, labels_of(visits_t, positives_t, parity))
        high = label >> 6
        low = label & 63
        notes = jnp.where(lane == 2 * parity, high.astype(jnp.float32), notes)
        notes = jnp.where(lane == 2 * parity + 1, low.astype(jnp.float32), notes)
        if parity == 0:
            filled = jnp.dot(as_bf16(chosen), queries_ref[...], preferred_element_type=jnp.float32)
            box_ref[:, :D] = filled.astype(bf)
    box_ref[:, D:] = notes.astype(bf)
    raw_ref[:NQ] = queries_ref[...]
    values = visits_t.astype(jnp.float32)
    parts = [values[k : k + 1, :] for k in range(VISITS)]
    row = jnp.concatenate(parts + [jnp.zeros((1, D - VISITS * NQ), jnp.float32)], axis=1)
    raw_ref[NQ:] = jnp.concatenate([row, jnp.zeros((EXTRA - 1, D), jnp.float32)], axis=0).astype(bf)


def all_kernel(*refs):
    box_ref = refs[LAB]
    for k in range(LAB):
        extra = refs[k][NQ:].astype(jnp.float32)
        parts = [extra[0:1, j * NQ : (j + 1) * NQ] for j in range(VISITS)]
        visits_t = jnp.concatenate(parts, axis=0).astype(jnp.int32)
        filled = jnp.dot(
            as_bf16(picks(visits_t, 1)), refs[k][:NQ], preferred_element_type=jnp.float32
        )
        box_ref[:, k] = filled.astype(jnp.bfloat16).reshape(CLUS, CAP, D)


def home_kernel(parity, visits_ref, homed_ref, before_ref, out_ref):
    chosen = as_bf16(picks(visits_ref[...], parity))
    out_ref[...] = before_ref[...] + lax.dot_general(
        chosen, homed_ref[...], (((0,), (0,)), ((), ())), preferred_element_type=jnp.float32
    )


def tile_grads(rows, high, low, first, w_ref):
    tag = (high * 64.0 + low).astype(jnp.int32) - first
    cols = []
    for c in range(0, LABELS, BAND):
        logits = lax.dot_general(
            rows,
            w_ref[0, c : c + BAND],
            (((1,), (1,)), ((), ())),
            preferred_element_type=jnp.float32,
        )
        place = lax.broadcasted_iota(jnp.int32, logits.shape, 1) + c
        target = jnp.where(tag == place, 1.0, 0.0)
        cols.append((jax.nn.sigmoid(logits) - target).astype(jnp.bfloat16))
    grad = jnp.concatenate(cols, axis=1)
    part = jnp.dot(grad, w_ref[0], preferred_element_type=jnp.float32)
    return grad, part.astype(jnp.bfloat16)


def first_kernel(lab_ref, rows_ref, w_ref, grad_ref, part_ref):
    for t in range(0, rows_ref.shape[0], TILE):
        notes = rows_ref[t : t + TILE, D:].astype(jnp.float32)
        grad, part = tile_grads(
            rows_ref[t : t + TILE, :D], notes[:, 0:1], notes[:, 1:2], lab_ref[0] * LABELS, w_ref
        )
        grad_ref[t : t + TILE] = grad
        part_ref[t : t + TILE] = part


def first_grads(lab, rows, weights):
    n = rows.shape[0]
    vmem = pltpu.VMEM
    return pl.pallas_call(
        first_kernel,
        grid=(1,),
        in_specs=[
            pl.BlockSpec(memory_space=pltpu.SMEM),
            pl.BlockSpec((n, D + TAGS), lambda i: (0, 0), memory_space=vmem),
            pl.BlockSpec((1, LABELS, D), lambda i: (0, 0, 0), memory_space=vmem),
        ],
        out_specs=(
            pl.BlockSpec((n, LABELS), lambda i: (0, 0), memory_space=vmem),
            pl.BlockSpec((n, D), lambda i: (0, 0), memory_space=vmem),
        ),
        out_shape=(
            jax.ShapeDtypeStruct((n, LABELS), jnp.bfloat16),
            jax.ShapeDtypeStruct((n, D), jnp.bfloat16),
        ),
        cost_estimate=pl.CostEstimate(
            flops=4 * n * LABELS * D, bytes_accessed=2 * n * 3000, transcendentals=n * LABELS
        ),
        name="first_grads",
    )(lab, rows, weights)


def second_kernel(lab_ref, rows_ref, own, low, high, far_a, far_b, w_ref, grad_ref, *parts):
    step = pl.program_id(0)
    early = step < STEPS // 2
    f32 = jnp.float32
    far = jnp.where(early, far_a[...].astype(f32), far_b[...].astype(f32))
    notes = [own[...].astype(f32), low[...].astype(f32), high[...].astype(f32), far]
    notes = jnp.stack([x.reshape(SRC, CAP, TAGS) for x in notes], axis=1).reshape(TILE, TAGS)
    rows = rows_ref[...].reshape(TILE, D)
    grad, part = tile_grads(rows, notes[:, 2:3], notes[:, 3:4], lab_ref[0] * LABELS, w_ref)
    grad_ref[...] = grad
    part = part.reshape(SRC, LAB, CAP, D)
    for k in range(3):
        parts[k][...] = part[:, k].reshape(SRC * CAP, D)

    @pl.when(early)
    def _():
        parts[3][...] = part[:, 3].reshape(SRC * CAP, D)

    @pl.when(jnp.logical_not(early))
    def _():
        parts[4][...] = part[:, 3].reshape(SRC * CAP, D)


def second_grads(lab, rows, pieces, weights):
    n = LAB * ROWS
    bf = jnp.bfloat16
    last = STEPS // 2 - 1
    here = SRC * CAP
    whole = lambda i: (i, D // TAGS)
    early = lambda i: (jnp.minimum(i, last), D // TAGS)
    late = lambda i: (jnp.maximum(i - last - 1, 0), D // TAGS)
    note = lambda at: pl.BlockSpec((here, TAGS), at)
    return pl.pallas_call(
        second_kernel,
        grid=(STEPS,),
        in_specs=[
            pl.BlockSpec(memory_space=pltpu.SMEM),
            pl.BlockSpec((SRC, LAB * CAP, D), lambda i: (i, 0, 0)),
            note(whole),
            note(whole),
            note(whole),
            note(early),
            note(late),
            pl.BlockSpec((1, LABELS, D), lambda i: (1, 0, 0)),
        ],
        out_specs=(
            pl.BlockSpec((TILE, LABELS), lambda i: (i, 0)),
            pl.BlockSpec((here, D), lambda i: (i, 0)),
            pl.BlockSpec((here, D), lambda i: (i, 0)),
            pl.BlockSpec((here, D), lambda i: (i, 0)),
            pl.BlockSpec((here, D), lambda i: (jnp.minimum(i, last), 0)),
            pl.BlockSpec((here, D), lambda i: (jnp.maximum(i - last - 1, 0), 0)),
        ),
        out_shape=(jax.ShapeDtypeStruct((n, LABELS), bf),)
        + (jax.ShapeDtypeStruct((ROWS, D), bf),) * 3
        + (jax.ShapeDtypeStruct((ROWS // 2, D), bf),) * 2,
        cost_estimate=pl.CostEstimate(
            flops=4 * n * LABELS * D, bytes_accessed=2 * n * 3000, transcendentals=n * LABELS
        ),
        name="second_grads",
    )(lab, rows, *pieces, weights)


def update_kernel(count, *refs):
    grads, rows = refs[:count], refs[count : 2 * count]
    w_ref, m_ref = refs[2 * count : 2 * count + 2]
    wo_ref, mo_ref = refs[-2:]
    fresh = momentum_decay * m_ref[0]
    for grad_ref, rows_ref in zip(grads, rows):
        fresh = fresh + lax.dot_general(
            grad_ref[...],
            rows_ref[:, :D],
            (((0,), (0,)), ((), ())),
            preferred_element_type=jnp.float32,
        )
    mo_ref[0] = fresh
    wo_ref[0] = (w_ref[0].astype(jnp.float32) - step_rate * fresh).astype(jnp.bfloat16)


def update(cluster, grads, rows, weights, momentum, before=()):
    bands = LABELS // BAND
    band = pl.BlockSpec((1, BAND, D), lambda b: (cluster, b, 0))
    n = sum(r.shape[0] for r in rows)
    count = len(grads)
    keep = [pl.BlockSpec(memory_space=pl.ANY) for _ in before]
    return pl.pallas_call(
        lambda *refs: update_kernel(count, *refs),
        grid=(bands,),
        in_specs=[pl.BlockSpec((g.shape[0], BAND), lambda b: (0, b)) for g in grads]
        + [pl.BlockSpec(r.shape, lambda b: (0, 0)) for r in rows]
        + [band, band]
        + keep,
        out_specs=(band, band),
        out_shape=(
            jax.ShapeDtypeStruct(weights.shape, weights.dtype),
            jax.ShapeDtypeStruct(momentum.shape, momentum.dtype),
        ),
        input_output_aliases={2 * count + 2 + k: k for k in range(len(before))},
        cost_estimate=pl.CostEstimate(
            flops=2 * n * LABELS * D, bytes_accessed=18 << 20, transcendentals=0
        ),
        name="update",
    )(*grads, *rows, weights, momentum, *before)


def swap(x):
    return lax.all_to_all(x, "clus", split_axis=0, concat_axis=0, tiled=True)


def add(*terms):
    total = terms[0].astype(jnp.float32)
    for term in terms[1:]:
        total = total + term.astype(jnp.float32)
    return total.astype(jnp.bfloat16)


def scatter_sum(own, low, high, far_a, far_b):
    half = ROWS // 2
    up = lax.ppermute(far_a, "lab", ring(1))
    down = lax.ppermute(far_b, "lab", ring(-1))
    up = jnp.concatenate([add(high[:half], up), high[half:]])
    down = jnp.concatenate([low[:half], add(low[half:], down)])
    up = lax.ppermute(up, "lab", ring(1))
    down = lax.ppermute(down, "lab", ring(-1))
    return own, up, down


def shards(queries, visits, positives, weights, momentum):
    vt, pt = visits.T, positives.T
    bf = jnp.bfloat16
    lab = lax.axis_index("lab").reshape(1).astype(jnp.int32)

    box_a, raw = pl.pallas_call(
        own_kernel,
        out_shape=(
            jax.ShapeDtypeStruct((ROWS, D + TAGS), bf),
            jax.ShapeDtypeStruct((NQ + EXTRA, D), bf),
        ),
        name="own_box",
    )(vt, pt, queries)
    peers = [raw] + [lax.ppermute(raw, "lab", ring(s)) for s in (1, -1, 2)]
    got_a = swap(box_a.reshape(CLUS, CAP, D + TAGS)).reshape(ROWS, D + TAGS)
    box_b = pl.pallas_call(
        all_kernel,
        out_shape=jax.ShapeDtypeStruct((CLUS, LAB, CAP, D), bf),
        name="all_box",
    )(*peers)
    got_a, box_b = lax.optimization_barrier((got_a, box_b))
    got_b = swap(box_b.reshape(CLUS, LAB * CAP, D))

    half = ROWS // 2
    from_low = lax.ppermute(got_a, "lab", ring(1))
    from_high = lax.ppermute(got_a, "lab", ring(-1))
    far_a = lax.ppermute(from_low[:half], "lab", ring(1))
    far_b = lax.ppermute(from_high[half:], "lab", ring(-1))
    pieces = (got_a, from_low, from_high, far_a, far_b)
    grads_a, parts_a = zip(*[first_grads(lab, p, weights) for p in pieces])
    own, up, down = scatter_sum(*parts_a)
    home_a = swap(add(own, up, down).reshape(CLUS, CAP, D)).reshape(ROWS, D)
    grad_b, *parts_b = second_grads(lab, got_b, pieces, weights)
    own, up, down = scatter_sum(*parts_b)
    new = update(0, grads_a, pieces, weights, momentum)
    new = update(1, (grad_b,), (got_b.reshape(LAB * ROWS, D),), weights, momentum, new)
    own, up, down, new = lax.optimization_barrier((own, up, down, new))
    home_b = swap(add(own, up, down).reshape(CLUS, CAP, D)).reshape(ROWS, D)

    total = jnp.zeros((NQ, D), jnp.float32)
    for parity, homed in ((0, home_a), (1, home_b)):
        total = pl.pallas_call(
            lambda *refs, parity=parity: home_kernel(parity, *refs),
            out_shape=jax.ShapeDtypeStruct((NQ, D), jnp.float32),
            name=f"home_{parity}",
        )(vt, homed, total)
    return (total, *new)


def solution(mesh):
    in_specs = (
        P(("clus", "lab"), None),
        P(("clus", "lab"), None),
        P(("clus", "lab"), None),
        P("clus", "lab", None),
        P("clus", "lab", None),
    )
    out_specs = (P(("clus", "lab"), None), P("clus", "lab", None), P("clus", "lab", None))
    return jax.shard_map(shards, mesh=mesh, in_specs=in_specs, out_specs=out_specs, check_vma=False)
```

```python
import jax
import jax.numpy as jnp
from jax import lax
from jax.experimental import pallas as pl
from jax.experimental.pallas import tpu as pltpu
from jax.sharding import PartitionSpec as P


momentum_decay = 0.9
step_rate = 0.002

CLUS = 32
LAB = 4
CAP = 16
NQ = 128
VISITS = 4
D = 768
EXTRA = 8
TAGS = 128
LABELS = 1024
BAND = 256
ROWS = CLUS * CAP


def ring(shift):
    return [(i, (i + shift) % LAB) for i in range(LAB)]


def picks(visits_t, parity):
    dest = lax.broadcasted_iota(jnp.int32, (CLUS, NQ), 0) * 2 + parity
    hit = visits_t[0:1, :] == dest
    for k in range(1, VISITS):
        hit = hit | (visits_t[k : k + 1, :] == dest)
    before = lax.broadcasted_iota(jnp.int32, (NQ, NQ), 0) < lax.broadcasted_iota(
        jnp.int32, (NQ, NQ), 1
    )
    rank = jnp.dot(
        hit.astype(jnp.float32).astype(jnp.bfloat16),
        before.astype(jnp.float32).astype(jnp.bfloat16),
        preferred_element_type=jnp.float32,
    )
    place = jnp.where(hit, rank, -1.0).astype(jnp.int32)
    slot = lax.broadcasted_iota(jnp.int32, (CLUS, CAP, NQ), 1)
    return (place[:, None, :] == slot).reshape(ROWS, NQ)


def as_bf16(flags):
    return flags.astype(jnp.float32).astype(jnp.bfloat16)


def labels_of(visits_t, positives_t, parity):
    dest = lax.broadcasted_iota(jnp.int32, (CLUS, NQ), 0) * 2 + parity
    label = jnp.zeros((CLUS, NQ), jnp.int32)
    for k in range(VISITS):
        label = label + jnp.where(visits_t[k : k + 1, :] == dest, positives_t[k : k + 1, :] + 1, 0)
    return label


def slot_labels(chosen, label):
    wide = jnp.broadcast_to(label[:, None, :], (CLUS, CAP, NQ)).reshape(ROWS, NQ)
    return jnp.sum(jnp.where(chosen, wide, 0), axis=1, keepdims=True) - 1


def own_kernel(visits_ref, positives_ref, queries_ref, box_ref, raw_ref):
    bf = jnp.bfloat16
    visits_t, positives_t = visits_ref[...], positives_ref[...]
    lane = lax.broadcasted_iota(jnp.int32, (ROWS, TAGS), 1)
    notes = jnp.zeros((ROWS, TAGS), jnp.float32)
    for parity in range(2):
        chosen = picks(visits_t, parity)
        label = slot_labels(chosen, labels_of(visits_t, positives_t, parity))
        high = label >> 6
        low = label & 63
        notes = jnp.where(lane == 2 * parity, high.astype(jnp.float32), notes)
        notes = jnp.where(lane == 2 * parity + 1, low.astype(jnp.float32), notes)
        if parity == 0:
            filled = jnp.dot(as_bf16(chosen), queries_ref[...], preferred_element_type=jnp.float32)
            box_ref[:, :D] = filled.astype(bf)
    box_ref[:, D:] = notes.astype(bf)
    raw_ref[:NQ] = queries_ref[...]
    values = visits_t.astype(jnp.float32)
    parts = [values[k : k + 1, :] for k in range(VISITS)]
    row = jnp.concatenate(parts + [jnp.zeros((1, D - VISITS * NQ), jnp.float32)], axis=1)
    raw_ref[NQ:] = jnp.concatenate([row, jnp.zeros((EXTRA - 1, D), jnp.float32)], axis=0).astype(bf)


def all_kernel(*refs):
    box_ref = refs[LAB]
    for k in range(LAB):
        extra = refs[k][NQ:].astype(jnp.float32)
        parts = [extra[0:1, j * NQ : (j + 1) * NQ] for j in range(VISITS)]
        visits_t = jnp.concatenate(parts, axis=0).astype(jnp.int32)
        filled = jnp.dot(
            as_bf16(picks(visits_t, 1)), refs[k][:NQ], preferred_element_type=jnp.float32
        )
        box_ref[:, k] = filled.astype(jnp.bfloat16).reshape(CLUS, CAP, D)


def home_kernel(visits_ref, homed_ref, out_ref):
    total = jnp.zeros((NQ, D), jnp.float32)
    for parity in range(2):
        chosen = as_bf16(picks(visits_ref[...], parity))
        rows = homed_ref[:, parity * D : (parity + 1) * D]
        total = total + lax.dot_general(
            chosen, rows, (((0,), (0,)), ((), ())), preferred_element_type=jnp.float32
        )
    out_ref[...] = total


def update_kernel(gn_ref, gf_ref, gb_ref, rn_ref, rf_ref, rb_ref, w_ref, m_ref, wo_ref, mo_ref):
    def apply(pairs):
        fresh = momentum_decay * m_ref[0]
        for grad_ref, rows_ref in pairs:
            fresh = fresh + lax.dot_general(
                grad_ref[...],
                rows_ref[...],
                (((0,), (0,)), ((), ())),
                preferred_element_type=jnp.float32,
            )
        mo_ref[0] = fresh
        wo_ref[0] = (w_ref[0].astype(jnp.float32) - step_rate * fresh).astype(jnp.bfloat16)

    @pl.when(pl.program_id(0) == 0)
    def _():
        apply(((gn_ref, rn_ref), (gf_ref, rf_ref)))

    @pl.when(pl.program_id(0) == 1)
    def _():
        apply(((gb_ref, rb_ref),))


def update(grad_a, grad_b, rows_a, rows_b, weights, momentum):
    bands = LABELS // BAND
    n = LAB * ROWS
    whole = lambda x: pl.BlockSpec(x.shape, lambda c, b: (0, 0))
    first = lambda x: pl.BlockSpec(
        (x.shape[0], BAND), lambda c, b: (0, b * (1 - c) + (bands - 1) * c)
    )
    band = pl.BlockSpec((1, BAND, D), lambda c, b: (c, b, 0))
    return pl.pallas_call(
        update_kernel,
        grid=(2, bands),
        in_specs=[first(g) for g in grad_a]
        + [pl.BlockSpec((n, BAND), lambda c, b: (0, b * c))]
        + [whole(r) for r in rows_a]
        + [whole(rows_b), band, band],
        out_specs=(band, band),
        out_shape=(
            jax.ShapeDtypeStruct(weights.shape, weights.dtype),
            jax.ShapeDtypeStruct(momentum.shape, momentum.dtype),
        ),
        compiler_params=pltpu.CompilerParams(
            dimension_semantics=("arbitrary", "arbitrary"), vmem_limit_bytes=56 << 20
        ),
        cost_estimate=pl.CostEstimate(
            flops=2 * 2 * n * LABELS * D, bytes_accessed=36 << 20, transcendentals=0
        ),
        name="update",
    )(*grad_a, grad_b, *rows_a, rows_b, weights, momentum)


def grads(rows, tag, weights, offsets):
    logits = jnp.einsum("rd,bd->rb", rows, weights, preferred_element_type=jnp.float32)
    target = (tag == offsets[None, :]).astype(jnp.float32)
    grad = (jax.nn.sigmoid(logits) - target).astype(jnp.bfloat16)
    part = jnp.einsum("rb,bd->rd", grad, weights, preferred_element_type=jnp.float32)
    return grad, part.astype(jnp.bfloat16)


def swap(x):
    return lax.all_to_all(x, "clus", split_axis=0, concat_axis=0, tiled=True)


def add(*terms):
    total = terms[0].astype(jnp.float32)
    for term in terms[1:]:
        total = total + term.astype(jnp.float32)
    return total.astype(jnp.bfloat16)


def ring_sum(parts):
    own, low, high, far = parts
    half = ROWS // 2
    up = lax.ppermute(far[:half], "lab", ring(1))
    down = lax.ppermute(far[half:], "lab", ring(-1))
    up = jnp.concatenate([add(high[:half], up), high[half:]])
    down = jnp.concatenate([low[:half], add(low[half:], down)])
    up = lax.ppermute(up, "lab", ring(1))
    down = lax.ppermute(down, "lab", ring(-1))
    return add(own, up, down)


def step(queries, visits, positives, weights, momentum):
    vt, pt = visits.T, positives.T
    bf = jnp.bfloat16
    me = lax.axis_index("lab")

    box_a, raw = pl.pallas_call(
        own_kernel,
        out_shape=(
            jax.ShapeDtypeStruct((ROWS, D + TAGS), bf),
            jax.ShapeDtypeStruct((NQ + EXTRA, D), bf),
        ),
        name="own_box",
    )(vt, pt, queries)
    peers = [raw] + [lax.ppermute(raw, "lab", ring(s)) for s in (1, -1, 2)]
    got_a = swap(box_a.reshape(CLUS, CAP, D + TAGS)).reshape(ROWS, D + TAGS)
    box_b = pl.pallas_call(
        all_kernel,
        out_shape=jax.ShapeDtypeStruct((CLUS, LAB, CAP, D), bf),
        name="all_box",
    )(*peers)
    got_a, box_b = lax.optimization_barrier((got_a, box_b))
    got_b = swap(box_b.reshape(CLUS, LAB * CAP, D)).reshape(LAB * ROWS, D)

    half = ROWS // 2
    from_low = lax.ppermute(got_a, "lab", ring(1))
    from_high = lax.ppermute(got_a, "lab", ring(-1))
    far_low = lax.ppermute(from_low[:half], "lab", ring(1))
    far_high = lax.ppermute(from_high[half:], "lab", ring(-1))
    near, far = (got_a, from_low, from_high), (far_low, far_high)
    rows_a = [jnp.concatenate([p[:, :D] for p in ps]) for ps in (near, far)]
    notes = [jnp.concatenate([p[:, D : D + 4] for p in ps]).astype(jnp.int32) for ps in (near, far)]
    tag_a = [x[:, 0:1] * 64 + x[:, 1:2] for x in notes]
    tag_b = jnp.concatenate([x[:, 2:3] * 64 + x[:, 3:4] for x in notes])
    tag_b = jnp.moveaxis(tag_b.reshape(LAB, CLUS, CAP), 0, 1).reshape(LAB * ROWS, 1)

    offsets = me * LABELS + jnp.arange(LABELS, dtype=jnp.int32)
    grad_far, part_far = grads(rows_a[1], tag_a[1], weights[0], offsets)
    grad_near, part_near = grads(rows_a[0], tag_a[0], weights[0], offsets)
    part_near = part_near.reshape(LAB - 1, ROWS, D)
    home_a = ring_sum((part_near[0], part_near[1], part_near[2], part_far))
    grad_b, part_b = grads(got_b, tag_b, weights[1], offsets)
    part_b = part_b.reshape(CLUS, LAB, CAP, D)
    home_b = ring_sum([part_b[:, k].reshape(ROWS, D) for k in range(LAB)])
    both = jnp.concatenate([home_a, home_b], axis=1).reshape(CLUS, CAP, 2 * D)
    both = swap(both).reshape(ROWS, 2 * D)
    weights_new, momentum_new = update(
        (grad_near, grad_far), grad_b, rows_a, got_b, weights, momentum
    )
    query_grad = pl.pallas_call(
        home_kernel, out_shape=jax.ShapeDtypeStruct((NQ, D), jnp.float32), name="home_sum"
    )(vt, both)
    return (query_grad, weights_new, momentum_new)


def solution(mesh):
    in_specs = (
        P(("clus", "lab"), None),
        P(("clus", "lab"), None),
        P(("clus", "lab"), None),
        P("clus", "lab", None),
        P("clus", "lab", None),
    )
    out_specs = (P(("clus", "lab"), None), P("clus", "lab", None), P("clus", "lab", None))
    return jax.shard_map(step, mesh=mesh, in_specs=in_specs, out_specs=out_specs, check_vma=False)
```

```python
import jax
import jax.numpy as jnp
from jax import lax
from jax.experimental import pallas as pl
from jax.experimental.pallas import tpu as pltpu
from jax.sharding import PartitionSpec as P


momentum_decay = 0.9
step_rate = 0.002

CLUS = 32
LAB = 4
CAP = 16
NQ = 128
VISITS = 4
D = 768
EXTRA = 8
TAGS = 128
LABELS = 1024
BAND = 256
ROWS = CLUS * CAP


def ring(shift):
    return [(i, (i + shift) % LAB) for i in range(LAB)]


def picks(visits_t, parity):
    dest = lax.broadcasted_iota(jnp.int32, (CLUS, NQ), 0) * 2 + parity
    hit = visits_t[0:1, :] == dest
    for k in range(1, VISITS):
        hit = hit | (visits_t[k : k + 1, :] == dest)
    before = lax.broadcasted_iota(jnp.int32, (NQ, NQ), 0) < lax.broadcasted_iota(
        jnp.int32, (NQ, NQ), 1
    )
    rank = jnp.dot(
        hit.astype(jnp.float32).astype(jnp.bfloat16),
        before.astype(jnp.float32).astype(jnp.bfloat16),
        preferred_element_type=jnp.float32,
    )
    place = jnp.where(hit, rank, -1.0).astype(jnp.int32)
    slot = lax.broadcasted_iota(jnp.int32, (CLUS, CAP, NQ), 1)
    return (place[:, None, :] == slot).reshape(ROWS, NQ)


def as_bf16(flags):
    return flags.astype(jnp.float32).astype(jnp.bfloat16)


def labels_of(visits_t, positives_t, parity):
    dest = lax.broadcasted_iota(jnp.int32, (CLUS, NQ), 0) * 2 + parity
    label = jnp.zeros((CLUS, NQ), jnp.int32)
    for k in range(VISITS):
        label = label + jnp.where(visits_t[k : k + 1, :] == dest, positives_t[k : k + 1, :] + 1, 0)
    return label


def slot_labels(chosen, label):
    wide = jnp.broadcast_to(label[:, None, :], (CLUS, CAP, NQ)).reshape(ROWS, NQ)
    return jnp.sum(jnp.where(chosen, wide, 0), axis=1, keepdims=True) - 1


def own_kernel(visits_ref, positives_ref, queries_ref, box_ref, raw_ref):
    bf = jnp.bfloat16
    visits_t, positives_t = visits_ref[...], positives_ref[...]
    lane = lax.broadcasted_iota(jnp.int32, (ROWS, TAGS), 1)
    notes = jnp.zeros((ROWS, TAGS), jnp.float32)
    for parity in range(2):
        chosen = picks(visits_t, parity)
        label = slot_labels(chosen, labels_of(visits_t, positives_t, parity))
        high = label >> 6
        low = label & 63
        notes = jnp.where(lane == 2 * parity, high.astype(jnp.float32), notes)
        notes = jnp.where(lane == 2 * parity + 1, low.astype(jnp.float32), notes)
        if parity == 0:
            filled = jnp.dot(as_bf16(chosen), queries_ref[...], preferred_element_type=jnp.float32)
            box_ref[:, :D] = filled.astype(bf)
    box_ref[:, D:] = notes.astype(bf)
    raw_ref[:NQ] = queries_ref[...]
    values = visits_t.astype(jnp.float32)
    parts = [values[k : k + 1, :] for k in range(VISITS)]
    row = jnp.concatenate(parts + [jnp.zeros((1, D - VISITS * NQ), jnp.float32)], axis=1)
    raw_ref[NQ:] = jnp.concatenate([row, jnp.zeros((EXTRA - 1, D), jnp.float32)], axis=0).astype(bf)


def all_kernel(*refs):
    box_ref = refs[LAB]
    for k in range(LAB):
        extra = refs[k][NQ:].astype(jnp.float32)
        parts = [extra[0:1, j * NQ : (j + 1) * NQ] for j in range(VISITS)]
        visits_t = jnp.concatenate(parts, axis=0).astype(jnp.int32)
        filled = jnp.dot(
            as_bf16(picks(visits_t, 1)), refs[k][:NQ], preferred_element_type=jnp.float32
        )
        box_ref[:, k] = filled.astype(jnp.bfloat16).reshape(CLUS, CAP, D)


def home_kernel(visits_ref, homed_ref, out_ref):
    total = jnp.zeros((NQ, D), jnp.float32)
    for parity in range(2):
        chosen = as_bf16(picks(visits_ref[...], parity))
        rows = homed_ref[:, parity * D : (parity + 1) * D]
        total = total + lax.dot_general(
            chosen, rows, (((0,), (0,)), ((), ())), preferred_element_type=jnp.float32
        )
    out_ref[...] = total


def update_kernel(*refs):
    ga, gb, ra, rb = refs[:LAB], refs[LAB], refs[LAB + 1 : 2 * LAB + 1], refs[2 * LAB + 1]
    w_ref, m_ref, wo_ref, mo_ref = refs[2 * LAB + 2 :]

    def apply(pairs):
        fresh = momentum_decay * m_ref[0]
        for grad_ref, rows_ref in pairs:
            fresh = fresh + lax.dot_general(
                grad_ref[...],
                rows_ref[...],
                (((0,), (0,)), ((), ())),
                preferred_element_type=jnp.float32,
            )
        mo_ref[0] = fresh
        wo_ref[0] = (w_ref[0].astype(jnp.float32) - step_rate * fresh).astype(jnp.bfloat16)

    @pl.when(pl.program_id(0) == 0)
    def _():
        apply(tuple(zip(ga, ra)))

    @pl.when(pl.program_id(0) == 1)
    def _():
        apply(((gb, rb),))


def update(grad_a, grad_b, rows_a, rows_b, weights, momentum):
    bands = LABELS // BAND
    n = LAB * ROWS
    whole = lambda x: pl.BlockSpec(x.shape, lambda c, b: (0, 0))
    first = lambda x: pl.BlockSpec(
        (x.shape[0], BAND), lambda c, b: (0, b * (1 - c) + (bands - 1) * c)
    )
    band = pl.BlockSpec((1, BAND, D), lambda c, b: (c, b, 0))
    return pl.pallas_call(
        update_kernel,
        grid=(2, bands),
        in_specs=[first(g) for g in grad_a]
        + [pl.BlockSpec((n, BAND), lambda c, b: (0, b * c))]
        + [whole(r) for r in rows_a]
        + [whole(rows_b), band, band],
        out_specs=(band, band),
        out_shape=(
            jax.ShapeDtypeStruct(weights.shape, weights.dtype),
            jax.ShapeDtypeStruct(momentum.shape, momentum.dtype),
        ),
        compiler_params=pltpu.CompilerParams(
            dimension_semantics=("arbitrary", "arbitrary"), vmem_limit_bytes=56 << 20
        ),
        cost_estimate=pl.CostEstimate(
            flops=2 * 2 * n * LABELS * D, bytes_accessed=36 << 20, transcendentals=0
        ),
        name="update",
    )(*grad_a, grad_b, *rows_a, rows_b, weights, momentum)


def grads(rows, tag, weights, offsets):
    logits = jnp.einsum("rd,bd->rb", rows, weights, preferred_element_type=jnp.float32)
    target = (tag == offsets[None, :]).astype(jnp.float32)
    grad = (jax.nn.sigmoid(logits) - target).astype(jnp.bfloat16)
    part = jnp.einsum("rb,bd->rd", grad, weights, preferred_element_type=jnp.float32)
    return grad, part.astype(jnp.bfloat16)


def swap(x):
    return lax.all_to_all(x, "clus", split_axis=0, concat_axis=0, tiled=True)


def add(*terms):
    total = terms[0].astype(jnp.float32)
    for term in terms[1:]:
        total = total + term.astype(jnp.float32)
    return total.astype(jnp.bfloat16)


def ring_sum(parts):
    own, low, high, far = parts
    half = ROWS // 2
    up = lax.ppermute(far[:half], "lab", ring(1))
    down = lax.ppermute(far[half:], "lab", ring(-1))
    up = jnp.concatenate([add(high[:half], up), high[half:]])
    down = jnp.concatenate([low[:half], add(low[half:], down)])
    up = lax.ppermute(up, "lab", ring(1))
    down = lax.ppermute(down, "lab", ring(-1))
    return add(own, up, down)


def step(queries, visits, positives, weights, momentum):
    vt, pt = visits.T, positives.T
    bf = jnp.bfloat16
    me = lax.axis_index("lab")

    box_a, raw = pl.pallas_call(
        own_kernel,
        out_shape=(
            jax.ShapeDtypeStruct((ROWS, D + TAGS), bf),
            jax.ShapeDtypeStruct((NQ + EXTRA, D), bf),
        ),
        name="own_box",
    )(vt, pt, queries)
    peers = [raw] + [lax.ppermute(raw, "lab", ring(s)) for s in (1, -1, 2)]
    got_a = swap(box_a.reshape(CLUS, CAP, D + TAGS)).reshape(ROWS, D + TAGS)
    box_b = pl.pallas_call(
        all_kernel,
        out_shape=jax.ShapeDtypeStruct((CLUS, LAB, CAP, D), bf),
        name="all_box",
    )(*peers)
    got_a, box_b = lax.optimization_barrier((got_a, box_b))
    got_b = swap(box_b.reshape(CLUS, LAB * CAP, D)).reshape(LAB * ROWS, D)

    half = ROWS // 2
    low_a = lax.ppermute(got_a[:half], "lab", ring(1))
    high_b = lax.ppermute(got_a[half:], "lab", ring(-1))
    low_b = lax.ppermute(got_a[half:], "lab", ring(1))
    high_a = lax.ppermute(got_a[:half], "lab", ring(-1))
    far_a = lax.ppermute(low_a, "lab", ring(1))
    far_b = lax.ppermute(high_b, "lab", ring(-1))
    blocks = ((got_a,), (low_a, low_b), (high_a, high_b), (far_a, far_b))
    offsets = me * LABELS + jnp.arange(LABELS, dtype=jnp.int32)
    rows_a, grads_a, parts_a, tags_b = [], [], [], []
    for block in blocks:
        rows = jnp.concatenate([p[:, :D] for p in block])
        notes = jnp.concatenate([p[:, D : D + 4] for p in block]).astype(jnp.int32)
        grad, part = grads(rows, notes[:, 0:1] * 64 + notes[:, 1:2], weights[0], offsets)
        rows_a.append(rows)
        grads_a.append(grad)
        parts_a.append(part)
        tags_b.append((notes[:, 2] * 64 + notes[:, 3]).reshape(CLUS, CAP))
    tag_b = jnp.stack(tags_b, axis=1).reshape(LAB * ROWS, 1)
    home_a = ring_sum(parts_a)
    grad_b, part_b = grads(got_b, tag_b, weights[1], offsets)
    part_b = part_b.reshape(CLUS, LAB, CAP, D)
    home_b = ring_sum([part_b[:, k].reshape(ROWS, D) for k in range(LAB)])
    both = jnp.concatenate([home_a, home_b], axis=1).reshape(CLUS, CAP, 2 * D)
    both = swap(both).reshape(ROWS, 2 * D)
    weights_new, momentum_new = update(grads_a, grad_b, rows_a, got_b, weights, momentum)
    query_grad = pl.pallas_call(
        home_kernel, out_shape=jax.ShapeDtypeStruct((NQ, D), jnp.float32), name="home_sum"
    )(vt, both)
    return (query_grad, weights_new, momentum_new)


def solution(mesh):
    in_specs = (
        P(("clus", "lab"), None),
        P(("clus", "lab"), None),
        P(("clus", "lab"), None),
        P("clus", "lab", None),
        P("clus", "lab", None),
    )
    out_specs = (P(("clus", "lab"), None), P("clus", "lab", None), P("clus", "lab", None))
    return jax.shard_map(step, mesh=mesh, in_specs=in_specs, out_specs=out_specs, check_vma=False)
```

```python
import jax
import jax.numpy as jnp
from jax import lax
from jax.experimental import pallas as pl
from jax.experimental.pallas import tpu as pltpu
from jax.sharding import PartitionSpec as P


momentum_decay = 0.9
step_rate = 0.002

CLUS = 32
LAB = 4
CAP = 16
NQ = 128
VISITS = 4
D = 768
EXTRA = 8
TAGS = 128
TILE = 256
SRC = TILE // (LAB * CAP)
STEPS = CLUS // SRC
LABELS = 1024
BAND = 256
ROWS = CLUS * CAP


def ring(shift):
    return [(i, (i + shift) % LAB) for i in range(LAB)]


def picks(visits_t, parity):
    dest = lax.broadcasted_iota(jnp.int32, (CLUS, NQ), 0) * 2 + parity
    hit = visits_t[0:1, :] == dest
    for k in range(1, VISITS):
        hit = hit | (visits_t[k : k + 1, :] == dest)
    before = lax.broadcasted_iota(jnp.int32, (NQ, NQ), 0) < lax.broadcasted_iota(
        jnp.int32, (NQ, NQ), 1
    )
    rank = jnp.dot(
        hit.astype(jnp.float32).astype(jnp.bfloat16),
        before.astype(jnp.float32).astype(jnp.bfloat16),
        preferred_element_type=jnp.float32,
    )
    place = jnp.where(hit, rank, -1.0).astype(jnp.int32)
    slot = lax.broadcasted_iota(jnp.int32, (CLUS, CAP, NQ), 1)
    return (place[:, None, :] == slot).reshape(ROWS, NQ)


def as_bf16(flags):
    return flags.astype(jnp.float32).astype(jnp.bfloat16)


def labels_of(visits_t, positives_t, parity):
    dest = lax.broadcasted_iota(jnp.int32, (CLUS, NQ), 0) * 2 + parity
    label = jnp.zeros((CLUS, NQ), jnp.int32)
    for k in range(VISITS):
        label = label + jnp.where(visits_t[k : k + 1, :] == dest, positives_t[k : k + 1, :] + 1, 0)
    return label


def slot_labels(chosen, label):
    wide = jnp.broadcast_to(label[:, None, :], (CLUS, CAP, NQ)).reshape(ROWS, NQ)
    return jnp.sum(jnp.where(chosen, wide, 0), axis=1, keepdims=True) - 1


def own_kernel(visits_ref, positives_ref, queries_ref, box_ref, raw_ref):
    bf = jnp.bfloat16
    visits_t, positives_t = visits_ref[...], positives_ref[...]
    lane = lax.broadcasted_iota(jnp.int32, (ROWS, TAGS), 1)
    notes = jnp.zeros((ROWS, TAGS), jnp.float32)
    for parity in range(2):
        chosen = picks(visits_t, parity)
        label = slot_labels(chosen, labels_of(visits_t, positives_t, parity))
        high = label >> 6
        low = label & 63
        notes = jnp.where(lane == 2 * parity, high.astype(jnp.float32), notes)
        notes = jnp.where(lane == 2 * parity + 1, low.astype(jnp.float32), notes)
        if parity == 0:
            filled = jnp.dot(as_bf16(chosen), queries_ref[...], preferred_element_type=jnp.float32)
            box_ref[:, :D] = filled.astype(bf)
    box_ref[:, D:] = notes.astype(bf)
    raw_ref[:NQ] = queries_ref[...]
    values = visits_t.astype(jnp.float32)
    parts = [values[k : k + 1, :] for k in range(VISITS)]
    row = jnp.concatenate(parts + [jnp.zeros((1, D - VISITS * NQ), jnp.float32)], axis=1)
    raw_ref[NQ:] = jnp.concatenate([row, jnp.zeros((EXTRA - 1, D), jnp.float32)], axis=0).astype(bf)


def all_kernel(*refs):
    box_ref = refs[LAB]
    for k in range(LAB):
        extra = refs[k][NQ:].astype(jnp.float32)
        parts = [extra[0:1, j * NQ : (j + 1) * NQ] for j in range(VISITS)]
        visits_t = jnp.concatenate(parts, axis=0).astype(jnp.int32)
        filled = jnp.dot(
            as_bf16(picks(visits_t, 1)), refs[k][:NQ], preferred_element_type=jnp.float32
        )
        box_ref[:, k] = filled.astype(jnp.bfloat16).reshape(CLUS, CAP, D)


def home_kernel(visits_ref, homed_ref, out_ref):
    total = jnp.zeros((NQ, D), jnp.float32)
    for parity in range(2):
        chosen = as_bf16(picks(visits_ref[...], parity))
        rows = homed_ref[:, parity * D : (parity + 1) * D]
        total = total + lax.dot_general(
            chosen, rows, (((0,), (0,)), ((), ())), preferred_element_type=jnp.float32
        )
    out_ref[...] = total


def tile_grads(rows, high, low, first, w_ref):
    tag = (high * 64.0 + low).astype(jnp.int32) - first
    cols = []
    for c in range(0, LABELS, BAND):
        logits = lax.dot_general(
            rows,
            w_ref[0, c : c + BAND],
            (((1,), (1,)), ((), ())),
            preferred_element_type=jnp.float32,
        )
        place = lax.broadcasted_iota(jnp.int32, logits.shape, 1) + c
        target = jnp.where(tag == place, 1.0, 0.0)
        cols.append((jax.nn.sigmoid(logits) - target).astype(jnp.bfloat16))
    grad = jnp.concatenate(cols, axis=1)
    part = jnp.dot(grad, w_ref[0], preferred_element_type=jnp.float32)
    return grad, part.astype(jnp.bfloat16)


def first_kernel(count, lab_ref, *refs):
    pieces, w_ref, grad_ref, parts = refs[:count], refs[count], refs[count + 1], refs[count + 2 :]
    at = 0
    for k, piece in enumerate(pieces):
        for t in range(0, piece.shape[0], TILE):
            notes = piece[t : t + TILE, D:].astype(jnp.float32)
            grad, part = tile_grads(
                piece[t : t + TILE, :D], notes[:, 0:1], notes[:, 1:2], lab_ref[0] * LABELS, w_ref
            )
            grad_ref[at : at + TILE] = grad
            if len(parts) == 1:
                parts[0][at : at + TILE] = part
            else:
                parts[k][t : t + TILE] = part
            at += TILE


def whole(shape):
    return pl.BlockSpec(shape, lambda *_: (0,) * len(shape))


def first_grads(lab, pieces, weights, apart=False):
    bf = jnp.bfloat16
    n = sum(p.shape[0] for p in pieces)
    sizes = [p.shape[0] for p in pieces] if apart else [n]
    count = len(pieces)
    return pl.pallas_call(
        lambda *refs: first_kernel(count, *refs),
        grid=(1,),
        in_specs=[pl.BlockSpec(memory_space=pltpu.SMEM)]
        + [whole(p.shape) for p in pieces]
        + [whole((1, LABELS, D))],
        out_specs=[whole((n, LABELS))] + [whole((m, D)) for m in sizes],
        out_shape=[jax.ShapeDtypeStruct((n, LABELS), bf)]
        + [jax.ShapeDtypeStruct((m, D), bf) for m in sizes],
        cost_estimate=pl.CostEstimate(
            flops=4 * n * LABELS * D, bytes_accessed=2 * n * 3000, transcendentals=n * LABELS
        ),
        name="first_grads",
    )(lab, *pieces, weights)


def second_kernel(lab_ref, rows_ref, *refs):
    notes_refs, w_ref, grad_ref, parts = refs[:7], refs[7], refs[8], refs[9:]
    step = pl.program_id(0)
    early = step < STEPS // 2
    f32 = jnp.float32
    notes = [notes_refs[0][...].astype(f32)]
    for k in range(1, 7, 2):
        notes.append(
            jnp.where(early, notes_refs[k][...].astype(f32), notes_refs[k + 1][...].astype(f32))
        )
    notes = jnp.stack([x.reshape(SRC, CAP, TAGS) for x in notes], axis=1).reshape(TILE, TAGS)
    rows = rows_ref[...].reshape(TILE, D)
    grad, part = tile_grads(rows, notes[:, 2:3], notes[:, 3:4], lab_ref[0] * LABELS, w_ref)
    grad_ref[...] = grad
    part = part.reshape(SRC, LAB, CAP, D)
    for k in range(3):
        parts[k][...] = part[:, k].reshape(SRC * CAP, D)

    @pl.when(early)
    def _():
        parts[3][...] = part[:, 3].reshape(SRC * CAP, D)

    @pl.when(jnp.logical_not(early))
    def _():
        parts[4][...] = part[:, 3].reshape(SRC * CAP, D)


def second_grads(lab, rows, pieces, weights):
    n = LAB * ROWS
    bf = jnp.bfloat16
    last = STEPS // 2 - 1
    here = SRC * CAP
    each = lambda i: (i, D // TAGS)
    early = lambda i: (jnp.minimum(i, last), D // TAGS)
    late = lambda i: (jnp.maximum(i - last - 1, 0), D // TAGS)
    note = lambda at: pl.BlockSpec((here, TAGS), at)
    return pl.pallas_call(
        second_kernel,
        grid=(STEPS,),
        in_specs=[
            pl.BlockSpec(memory_space=pltpu.SMEM),
            pl.BlockSpec((SRC, LAB * CAP, D), lambda i: (i, 0, 0)),
            note(each),
        ]
        + [note(early), note(late)] * 3
        + [pl.BlockSpec((1, LABELS, D), lambda i: (1, 0, 0))],
        out_specs=(
            pl.BlockSpec((TILE, LABELS), lambda i: (i, 0)),
            pl.BlockSpec((here, D), lambda i: (i, 0)),
            pl.BlockSpec((here, D), lambda i: (i, 0)),
            pl.BlockSpec((here, D), lambda i: (i, 0)),
            pl.BlockSpec((here, D), lambda i: (jnp.minimum(i, last), 0)),
            pl.BlockSpec((here, D), lambda i: (jnp.maximum(i - last - 1, 0), 0)),
        ),
        out_shape=(jax.ShapeDtypeStruct((n, LABELS), bf),)
        + (jax.ShapeDtypeStruct((ROWS, D), bf),) * 3
        + (jax.ShapeDtypeStruct((ROWS // 2, D), bf),) * 2,
        cost_estimate=pl.CostEstimate(
            flops=4 * n * LABELS * D, bytes_accessed=2 * n * 3000, transcendentals=n * LABELS
        ),
        name="second_grads",
    )(lab, rows, *pieces, weights)


def update_kernel(counts, *refs):
    grads, rest = refs[: len(counts)], refs[len(counts) :]
    rows, rest = rest[: sum(counts)], rest[sum(counts) :]
    w_ref, m_ref, wo_ref, mo_ref = rest[0], rest[1], rest[-2], rest[-1]
    fresh = momentum_decay * m_ref[0]
    k = 0
    for grad_ref, count in zip(grads, counts):
        at = 0
        for rows_ref in rows[k : k + count]:
            size = rows_ref.shape[0]
            fresh = fresh + lax.dot_general(
                grad_ref[at : at + size],
                rows_ref[:, :D],
                (((0,), (0,)), ((), ())),
                preferred_element_type=jnp.float32,
            )
            at += size
        k += count
    mo_ref[0] = fresh
    wo_ref[0] = (w_ref[0].astype(jnp.float32) - step_rate * fresh).astype(jnp.bfloat16)


def update(cluster, grads, blocks, weights, momentum, before=()):
    bands = LABELS // BAND
    band = pl.BlockSpec((1, BAND, D), lambda b: (cluster, b, 0))
    counts = tuple(len(block) for block in blocks)
    rows = [piece for block in blocks for piece in block]
    first = len(grads) + len(rows) + 2
    return pl.pallas_call(
        lambda *refs: update_kernel(counts, *refs),
        grid=(bands,),
        in_specs=[pl.BlockSpec((g.shape[0], BAND), lambda b: (0, b)) for g in grads]
        + [whole(r.shape) for r in rows]
        + [band, band]
        + [pl.BlockSpec(memory_space=pl.ANY) for _ in before],
        out_specs=(band, band),
        out_shape=(
            jax.ShapeDtypeStruct(weights.shape, weights.dtype),
            jax.ShapeDtypeStruct(momentum.shape, momentum.dtype),
        ),
        input_output_aliases={first + k: k for k in range(len(before))},
        cost_estimate=pl.CostEstimate(
            flops=2 * LAB * ROWS * LABELS * D, bytes_accessed=18 << 20, transcendentals=0
        ),
        name="update",
    )(*grads, *rows, weights, momentum, *before)


def swap(x):
    return lax.all_to_all(x, "clus", split_axis=0, concat_axis=0, tiled=True)


def add(*terms):
    total = terms[0].astype(jnp.float32)
    for term in terms[1:]:
        total = total + term.astype(jnp.float32)
    return total.astype(jnp.bfloat16)


def ring_sum(parts):
    own, low, high, far_a, far_b = parts
    half = ROWS // 2
    up = lax.ppermute(far_a, "lab", ring(1))
    down = lax.ppermute(far_b, "lab", ring(-1))
    up = jnp.concatenate([add(high[:half], up), high[half:]])
    down = jnp.concatenate([low[:half], add(low[half:], down)])
    up = lax.ppermute(up, "lab", ring(1))
    down = lax.ppermute(down, "lab", ring(-1))
    return add(own, up, down)


def step(queries, visits, positives, weights, momentum):
    vt, pt = visits.T, positives.T
    bf = jnp.bfloat16
    lab = lax.axis_index("lab").reshape(1).astype(jnp.int32)

    box_a, raw = pl.pallas_call(
        own_kernel,
        out_shape=(
            jax.ShapeDtypeStruct((ROWS, D + TAGS), bf),
            jax.ShapeDtypeStruct((NQ + EXTRA, D), bf),
        ),
        name="own_box",
    )(vt, pt, queries)
    peers = [raw] + [lax.ppermute(raw, "lab", ring(s)) for s in (1, -1, 2)]
    got_a = swap(box_a.reshape(CLUS, CAP, D + TAGS)).reshape(ROWS, D + TAGS)
    box_b = pl.pallas_call(
        all_kernel,
        out_shape=jax.ShapeDtypeStruct((CLUS, LAB, CAP, D), bf),
        name="all_box",
    )(*peers)
    got_a, box_b = lax.optimization_barrier((got_a, box_b))
    got_b = swap(box_b.reshape(CLUS, LAB * CAP, D))

    half = ROWS // 2
    low_a = lax.ppermute(got_a[:half], "lab", ring(1))
    high_b = lax.ppermute(got_a[half:], "lab", ring(-1))
    low_b = lax.ppermute(got_a[half:], "lab", ring(1))
    high_a = lax.ppermute(got_a[:half], "lab", ring(-1))
    far_a = lax.ppermute(low_a, "lab", ring(1))
    far_b = lax.ppermute(high_b, "lab", ring(-1))
    blocks = ((got_a,), (low_a, low_b), (high_a, high_b), (far_a, far_b))
    grads_a, parts_a = [], []
    for block, place in zip(blocks, ("here", "near1", "near2", "far")):
        grad, *parts = first_grads(lab, block, weights, apart=place == "far")
        grads_a.append(grad)
        parts_a += parts
    home_a = ring_sum(parts_a)
    pieces = [p for block in blocks for p in block]
    grad_b, *parts_b = second_grads(lab, got_b, pieces, weights)
    home_b = ring_sum(parts_b)
    both = jnp.concatenate([home_a, home_b], axis=1).reshape(CLUS, CAP, 2 * D)
    both = swap(both).reshape(ROWS, 2 * D)
    new = update(0, grads_a, blocks, weights, momentum)
    rows_b = ((got_b.reshape(LAB * ROWS, D),),)
    new = update(1, (grad_b,), rows_b, weights, momentum, new)
    query_grad = pl.pallas_call(
        home_kernel, out_shape=jax.ShapeDtypeStruct((NQ, D), jnp.float32), name="home_sum"
    )(vt, both)
    return (query_grad, *new)


def solution(mesh):
    in_specs = (
        P(("clus", "lab"), None),
        P(("clus", "lab"), None),
        P(("clus", "lab"), None),
        P("clus", "lab", None),
        P("clus", "lab", None),
    )
    out_specs = (P(("clus", "lab"), None), P("clus", "lab", None), P("clus", "lab", None))
    return jax.shard_map(step, mesh=mesh, in_specs=in_specs, out_specs=out_specs, check_vma=False)
```

```python
import jax
import jax.numpy as jnp
from jax import lax
from jax.experimental import pallas as pl
from jax.experimental.pallas import tpu as pltpu
from jax.sharding import PartitionSpec as P


momentum_decay = 0.9
step_rate = 0.002

CLUS = 32
LAB = 4
CAP = 16
NQ = 128
VISITS = 4
D = 768
EXTRA = 8
TAGS = 128
TILE = 256
LABELS = 1024
BAND = 256
ROWS = CLUS * CAP


def ring(shift):
    return [(i, (i + shift) % LAB) for i in range(LAB)]


def picks(visits_t, parity):
    dest = lax.broadcasted_iota(jnp.int32, (CLUS, NQ), 0) * 2 + parity
    hit = visits_t[0:1, :] == dest
    for k in range(1, VISITS):
        hit = hit | (visits_t[k : k + 1, :] == dest)
    before = lax.broadcasted_iota(jnp.int32, (NQ, NQ), 0) < lax.broadcasted_iota(
        jnp.int32, (NQ, NQ), 1
    )
    rank = jnp.dot(
        hit.astype(jnp.float32).astype(jnp.bfloat16),
        before.astype(jnp.float32).astype(jnp.bfloat16),
        preferred_element_type=jnp.float32,
    )
    place = jnp.where(hit, rank, -1.0).astype(jnp.int32)
    slot = lax.broadcasted_iota(jnp.int32, (CLUS, CAP, NQ), 1)
    return (place[:, None, :] == slot).reshape(ROWS, NQ)


def as_bf16(flags):
    return flags.astype(jnp.float32).astype(jnp.bfloat16)


def labels_of(visits_t, positives_t, parity):
    dest = lax.broadcasted_iota(jnp.int32, (CLUS, NQ), 0) * 2 + parity
    label = jnp.zeros((CLUS, NQ), jnp.int32)
    for k in range(VISITS):
        label = label + jnp.where(visits_t[k : k + 1, :] == dest, positives_t[k : k + 1, :] + 1, 0)
    return label


def slot_labels(chosen, label):
    wide = jnp.broadcast_to(label[:, None, :], (CLUS, CAP, NQ)).reshape(ROWS, NQ)
    return jnp.sum(jnp.where(chosen, wide, 0), axis=1, keepdims=True) - 1


def own_kernel(visits_ref, positives_ref, queries_ref, box_ref, raw_ref):
    bf = jnp.bfloat16
    visits_t, positives_t = visits_ref[...], positives_ref[...]
    lane = lax.broadcasted_iota(jnp.int32, (ROWS, TAGS), 1)
    notes = jnp.zeros((ROWS, TAGS), jnp.float32)
    for parity in range(2):
        chosen = picks(visits_t, parity)
        label = slot_labels(chosen, labels_of(visits_t, positives_t, parity))
        high = label >> 6
        low = label & 63
        notes = jnp.where(lane == 2 * parity, high.astype(jnp.float32), notes)
        notes = jnp.where(lane == 2 * parity + 1, low.astype(jnp.float32), notes)
        if parity == 0:
            filled = jnp.dot(as_bf16(chosen), queries_ref[...], preferred_element_type=jnp.float32)
            box_ref[:, :D] = filled.astype(bf)
    box_ref[:, D:] = notes.astype(bf)
    raw_ref[:NQ] = queries_ref[...]
    values = visits_t.astype(jnp.float32)
    parts = [values[k : k + 1, :] for k in range(VISITS)]
    row = jnp.concatenate(parts + [jnp.zeros((1, D - VISITS * NQ), jnp.float32)], axis=1)
    raw_ref[NQ:] = jnp.concatenate([row, jnp.zeros((EXTRA - 1, D), jnp.float32)], axis=0).astype(bf)


def all_kernel(*refs):
    box_ref = refs[LAB]
    for k in range(LAB):
        extra = refs[k][NQ:].astype(jnp.float32)
        parts = [extra[0:1, j * NQ : (j + 1) * NQ] for j in range(VISITS)]
        visits_t = jnp.concatenate(parts, axis=0).astype(jnp.int32)
        filled = jnp.dot(
            as_bf16(picks(visits_t, 1)), refs[k][:NQ], preferred_element_type=jnp.float32
        )
        box_ref[:, k] = filled.astype(jnp.bfloat16).reshape(CLUS, CAP, D)


def home_kernel(visits_ref, homed_ref, out_ref):
    total = jnp.zeros((NQ, D), jnp.float32)
    for parity in range(2):
        chosen = as_bf16(picks(visits_ref[...], parity))
        rows = homed_ref[:, parity * D : (parity + 1) * D]
        total = total + lax.dot_general(
            chosen, rows, (((0,), (0,)), ((), ())), preferred_element_type=jnp.float32
        )
    out_ref[...] = total


def tile_grads(rows, high, low, first, w_ref):
    tag = (high * 64.0 + low).astype(jnp.int32) - first
    cols = []
    for c in range(0, LABELS, BAND):
        logits = lax.dot_general(
            rows,
            w_ref[0, c : c + BAND],
            (((1,), (1,)), ((), ())),
            preferred_element_type=jnp.float32,
        )
        place = lax.broadcasted_iota(jnp.int32, logits.shape, 1) + c
        target = jnp.where(tag == place, 1.0, 0.0)
        cols.append((jax.nn.sigmoid(logits) - target).astype(jnp.bfloat16))
    grad = jnp.concatenate(cols, axis=1)
    part = jnp.dot(grad, w_ref[0], preferred_element_type=jnp.float32)
    return grad, part.astype(jnp.bfloat16)


def first_kernel(count, lab_ref, *refs):
    pieces, w_ref, grad_ref, parts = refs[:count], refs[count], refs[count + 1], refs[count + 2 :]
    at = 0
    for k, piece in enumerate(pieces):
        for t in range(0, piece.shape[0], TILE):
            notes = piece[t : t + TILE, D:].astype(jnp.float32)
            grad, part = tile_grads(
                piece[t : t + TILE, :D], notes[:, 0:1], notes[:, 1:2], lab_ref[0] * LABELS, w_ref
            )
            grad_ref[at : at + TILE] = grad
            if len(parts) == 1:
                parts[0][at : at + TILE] = part
            else:
                parts[k][t : t + TILE] = part
            at += TILE


def whole(shape):
    return pl.BlockSpec(shape, lambda *_: (0,) * len(shape))


def first_grads(lab, pieces, weights, apart=False):
    bf = jnp.bfloat16
    n = sum(p.shape[0] for p in pieces)
    sizes = [p.shape[0] for p in pieces] if apart else [n]
    count = len(pieces)
    return pl.pallas_call(
        lambda *refs: first_kernel(count, *refs),
        grid=(1,),
        in_specs=[pl.BlockSpec(memory_space=pltpu.SMEM)]
        + [whole(p.shape) for p in pieces]
        + [whole((1, LABELS, D))],
        out_specs=[whole((n, LABELS))] + [whole((m, D)) for m in sizes],
        out_shape=[jax.ShapeDtypeStruct((n, LABELS), bf)]
        + [jax.ShapeDtypeStruct((m, D), bf) for m in sizes],
        cost_estimate=pl.CostEstimate(
            flops=4 * n * LABELS * D, bytes_accessed=2 * n * 3000, transcendentals=n * LABELS
        ),
        name="first_grads",
    )(lab, *pieces, weights)


def second_kernel(near, lab_ref, rows_ref, *refs):
    count = 5 if near else 2
    notes_refs, w_ref, grad_ref, parts = refs[:count], refs[count], refs[count + 1], refs[count + 2 :]
    block, early = pl.program_id(0), pl.program_id(1) == 0
    notes = [ref[...].astype(jnp.float32) for ref in notes_refs]
    pair = lambda k: jnp.where(early, notes[k], notes[k + 1])
    if near:
        notes = jnp.where(block == 0, notes[0], jnp.where(block == 1, pair(1), pair(3)))
    else:
        notes = pair(0)
    rows = rows_ref[...].reshape(TILE, D)
    grad, part = tile_grads(rows, notes[:, 2:3], notes[:, 3:4], lab_ref[0] * LABELS, w_ref)
    grad_ref[...] = grad
    if near:
        parts[0][0] = part
        return

    @pl.when(early)
    def _():
        parts[0][...] = part

    @pl.when(jnp.logical_not(early))
    def _():
        parts[1][...] = part


def second_grads(lab, rows, blocks, weights, near):
    bf = jnp.bfloat16
    pieces = [p for block in blocks for p in block]
    first, count = (0, LAB - 1) if near else (LAB - 1, 1)
    n = count * ROWS
    source = TILE // CAP
    still = pl.BlockSpec((TILE, TAGS), lambda k, i: (0, D // TAGS))
    each = pl.BlockSpec((TILE, TAGS), lambda k, i: (i, D // TAGS))
    if near:
        part_specs = [pl.BlockSpec((1, TILE, D), lambda k, i: (k, i, 0))]
        part_shapes = [jax.ShapeDtypeStruct((count, ROWS, D), bf)]
    else:
        part_specs = [whole((TILE, D))] * 2
        part_shapes = [jax.ShapeDtypeStruct((TILE, D), bf)] * 2
    return pl.pallas_call(
        lambda *refs: second_kernel(near, *refs),
        grid=(count, 2),
        in_specs=[
            pl.BlockSpec(memory_space=pltpu.SMEM),
            pl.BlockSpec((source, CAP, D), lambda k, i: (i, first + k, 0)),
        ]
        + ([each] if near else [])
        + [still] * (4 if near else 2)
        + [pl.BlockSpec((1, LABELS, D), lambda k, i: (1, 0, 0))],
        out_specs=[pl.BlockSpec((TILE, LABELS), lambda k, i: (2 * k + i, 0))] + part_specs,
        out_shape=[jax.ShapeDtypeStruct((n, LABELS), bf)] + part_shapes,
        cost_estimate=pl.CostEstimate(
            flops=4 * n * LABELS * D, bytes_accessed=2 * n * 3000, transcendentals=n * LABELS
        ),
        name="second_grads",
    )(lab, rows, *pieces, weights)


def update_kernel(counts, *refs):
    grads, rest = refs[: len(counts)], refs[len(counts) :]
    many = max(sum(counts), 1)
    rows, rest = rest[:many], rest[many:]
    w_ref, m_ref, wo_ref, mo_ref = rest[0], rest[1], rest[-2], rest[-1]
    terms = []
    if sum(counts):
        k = 0
        for grad_ref, count in zip(grads, counts):
            at = 0
            for rows_ref in rows[k : k + count]:
                size = rows_ref.shape[0]
                terms.append((grad_ref[at : at + size], rows_ref[:, :D]))
                at += size
            k += count
    else:
        k = 0
        for grad_ref in grads:
            for at in range(0, grad_ref.shape[0], ROWS):
                slots = rows[0][:, k * CAP : (k + 1) * CAP].reshape(ROWS, D)
                terms.append((grad_ref[at : at + ROWS], slots))
                k += 1
    fresh = momentum_decay * m_ref[0]
    for grad, values in terms:
        fresh = fresh + lax.dot_general(
            grad, values, (((0,), (0,)), ((), ())), preferred_element_type=jnp.float32
        )
    mo_ref[0] = fresh
    wo_ref[0] = (w_ref[0].astype(jnp.float32) - step_rate * fresh).astype(jnp.bfloat16)


def update(cluster, grads, blocks, weights, momentum, before=()):
    bands = LABELS // BAND
    band = pl.BlockSpec((1, BAND, D), lambda b: (cluster, b, 0))
    shared = not isinstance(blocks, tuple)
    counts = (0,) * len(grads) if shared else tuple(len(block) for block in blocks)
    rows = [blocks] if shared else [piece for block in blocks for piece in block]
    first = len(grads) + len(rows) + 2
    return pl.pallas_call(
        lambda *refs: update_kernel(counts, *refs),
        grid=(bands,),
        in_specs=[pl.BlockSpec((g.shape[0], BAND), lambda b: (0, b)) for g in grads]
        + [whole(r.shape) for r in rows]
        + [band, band]
        + [pl.BlockSpec(memory_space=pl.ANY) for _ in before],
        out_specs=(band, band),
        out_shape=(
            jax.ShapeDtypeStruct(weights.shape, weights.dtype),
            jax.ShapeDtypeStruct(momentum.shape, momentum.dtype),
        ),
        input_output_aliases={first + k: k for k in range(len(before))},
        cost_estimate=pl.CostEstimate(
            flops=2 * LAB * ROWS * LABELS * D, bytes_accessed=18 << 20, transcendentals=0
        ),
        name="update",
    )(*grads, *rows, weights, momentum, *before)


def swap(x):
    return lax.all_to_all(x, "clus", split_axis=0, concat_axis=0, tiled=True)


def add(*terms):
    total = terms[0].astype(jnp.float32)
    for term in terms[1:]:
        total = total + term.astype(jnp.float32)
    return total.astype(jnp.bfloat16)


def ring_sum(parts):
    own, low, high, far_a, far_b = parts
    half = ROWS // 2
    up = lax.ppermute(far_a, "lab", ring(1))
    down = lax.ppermute(far_b, "lab", ring(-1))
    up = jnp.concatenate([add(high[:half], up), high[half:]])
    down = jnp.concatenate([low[:half], add(low[half:], down)])
    up = lax.ppermute(up, "lab", ring(1))
    down = lax.ppermute(down, "lab", ring(-1))
    return add(own, up, down)


def step(queries, visits, positives, weights, momentum):
    vt, pt = visits.T, positives.T
    bf = jnp.bfloat16
    lab = lax.axis_index("lab").reshape(1).astype(jnp.int32)

    box_a, raw = pl.pallas_call(
        own_kernel,
        out_shape=(
            jax.ShapeDtypeStruct((ROWS, D + TAGS), bf),
            jax.ShapeDtypeStruct((NQ + EXTRA, D), bf),
        ),
        name="own_box",
    )(vt, pt, queries)
    peers = [raw] + [lax.ppermute(raw, "lab", ring(s)) for s in (1, -1, 2)]
    got_a = swap(box_a.reshape(CLUS, CAP, D + TAGS)).reshape(ROWS, D + TAGS)
    box_b = pl.pallas_call(
        all_kernel,
        out_shape=jax.ShapeDtypeStruct((CLUS, LAB, CAP, D), bf),
        name="all_box",
    )(*peers)
    got_a, box_b = lax.optimization_barrier((got_a, box_b))
    got_b = swap(box_b.reshape(CLUS, LAB * CAP, D))

    half = ROWS // 2
    low_a = lax.ppermute(got_a[:half], "lab", ring(1))
    high_b = lax.ppermute(got_a[half:], "lab", ring(-1))
    low_b = lax.ppermute(got_a[half:], "lab", ring(1))
    high_a = lax.ppermute(got_a[:half], "lab", ring(-1))
    far_a = lax.ppermute(low_a, "lab", ring(1))
    far_b = lax.ppermute(high_b, "lab", ring(-1))
    blocks = ((got_a,), (low_a, low_b), (high_a, high_b), (far_a, far_b))
    grads_a, parts_a = [], []
    for block, place in zip(blocks, ("here", "near1", "near2", "far")):
        grad, *parts = first_grads(lab, block, weights, apart=place == "far")
        grads_a.append(grad)
        parts_a += parts
    home_a = ring_sum(parts_a)
    grad_far, *far_b_parts = second_grads(lab, got_b, blocks[3:], weights, near=False)
    grad_near, parts_near = second_grads(lab, got_b, blocks[:3], weights, near=True)
    home_b = ring_sum([parts_near[0], parts_near[1], parts_near[2]] + far_b_parts)
    both = jnp.concatenate([home_a, home_b], axis=1).reshape(CLUS, CAP, 2 * D)
    both = swap(both).reshape(ROWS, 2 * D)
    new = update(0, grads_a, blocks, weights, momentum)
    new = update(1, (grad_near, grad_far), got_b, weights, momentum, new)
    query_grad = pl.pallas_call(
        home_kernel, out_shape=jax.ShapeDtypeStruct((NQ, D), jnp.float32), name="home_sum"
    )(vt, both)
    return (query_grad, *new)


def solution(mesh):
    in_specs = (
        P(("clus", "lab"), None),
        P(("clus", "lab"), None),
        P(("clus", "lab"), None),
        P("clus", "lab", None),
        P("clus", "lab", None),
    )
    out_specs = (P(("clus", "lab"), None), P("clus", "lab", None), P("clus", "lab", None))
    return jax.shard_map(step, mesh=mesh, in_specs=in_specs, out_specs=out_specs, check_vma=False)
```

```python
import jax
import jax.numpy as jnp
from jax import lax
from jax.experimental import pallas as pl
from jax.experimental.pallas import tpu as pltpu
from jax.sharding import PartitionSpec as P


momentum_decay = 0.9
step_rate = 0.002

CLUS = 32
LAB = 4
CAP = 16
NQ = 128
VISITS = 4
D = 768
EXTRA = 8
TAGS = 128
TILE = 256
LABELS = 1024
BAND = 256
ROWS = CLUS * CAP


def ring(shift):
    return [(i, (i + shift) % LAB) for i in range(LAB)]


def picks(visits_t, parity):
    dest = lax.broadcasted_iota(jnp.int32, (CLUS, NQ), 0) * 2 + parity
    hit = visits_t[0:1, :] == dest
    for k in range(1, VISITS):
        hit = hit | (visits_t[k : k + 1, :] == dest)
    before = lax.broadcasted_iota(jnp.int32, (NQ, NQ), 0) < lax.broadcasted_iota(
        jnp.int32, (NQ, NQ), 1
    )
    rank = jnp.dot(
        hit.astype(jnp.float32).astype(jnp.bfloat16),
        before.astype(jnp.float32).astype(jnp.bfloat16),
        preferred_element_type=jnp.float32,
    )
    place = jnp.where(hit, rank, -1.0).astype(jnp.int32)
    slot = lax.broadcasted_iota(jnp.int32, (CLUS, CAP, NQ), 1)
    return (place[:, None, :] == slot).reshape(ROWS, NQ)


def as_bf16(flags):
    return flags.astype(jnp.float32).astype(jnp.bfloat16)


def labels_of(visits_t, positives_t, parity):
    dest = lax.broadcasted_iota(jnp.int32, (CLUS, NQ), 0) * 2 + parity
    label = jnp.zeros((CLUS, NQ), jnp.int32)
    for k in range(VISITS):
        label = label + jnp.where(visits_t[k : k + 1, :] == dest, positives_t[k : k + 1, :] + 1, 0)
    return label


def slot_labels(chosen, label):
    wide = jnp.broadcast_to(label[:, None, :], (CLUS, CAP, NQ)).reshape(ROWS, NQ)
    return jnp.sum(jnp.where(chosen, wide, 0), axis=1, keepdims=True) - 1


def own_kernel(visits_ref, positives_ref, queries_ref, box_ref, raw_ref):
    bf = jnp.bfloat16
    visits_t, positives_t = visits_ref[...], positives_ref[...]
    lane = lax.broadcasted_iota(jnp.int32, (ROWS, TAGS), 1)
    notes = jnp.zeros((ROWS, TAGS), jnp.float32)
    for parity in range(2):
        chosen = picks(visits_t, parity)
        label = slot_labels(chosen, labels_of(visits_t, positives_t, parity))
        high = label >> 6
        low = label & 63
        notes = jnp.where(lane == 2 * parity, high.astype(jnp.float32), notes)
        notes = jnp.where(lane == 2 * parity + 1, low.astype(jnp.float32), notes)
        if parity == 0:
            filled = jnp.dot(as_bf16(chosen), queries_ref[...], preferred_element_type=jnp.float32)
            box_ref[:, :D] = filled.astype(bf)
    box_ref[:, D:] = notes.astype(bf)
    raw_ref[:NQ] = queries_ref[...]
    values = visits_t.astype(jnp.float32)
    parts = [values[k : k + 1, :] for k in range(VISITS)]
    row = jnp.concatenate(parts + [jnp.zeros((1, D - VISITS * NQ), jnp.float32)], axis=1)
    raw_ref[NQ:] = jnp.concatenate([row, jnp.zeros((EXTRA - 1, D), jnp.float32)], axis=0).astype(bf)


def all_kernel(*refs):
    box_ref = refs[LAB]
    for k in range(LAB):
        extra = refs[k][NQ:].astype(jnp.float32)
        parts = [extra[0:1, j * NQ : (j + 1) * NQ] for j in range(VISITS)]
        visits_t = jnp.concatenate(parts, axis=0).astype(jnp.int32)
        filled = jnp.dot(
            as_bf16(picks(visits_t, 1)), refs[k][:NQ], preferred_element_type=jnp.float32
        )
        box_ref[:, k] = filled.astype(jnp.bfloat16).reshape(CLUS, CAP, D)


def home_kernel(parity, visits_ref, homed_ref, *refs):
    chosen = as_bf16(picks(visits_ref[...], parity))
    total = lax.dot_general(
        chosen, homed_ref[...], (((0,), (0,)), ((), ())), preferred_element_type=jnp.float32
    )
    for before_ref in refs[:-1]:
        total = total + before_ref[...]
    refs[-1][...] = total


def tile_grads(rows, high, low, first, w_ref):
    tag = (high * 64.0 + low).astype(jnp.int32) - first
    cols = []
    for c in range(0, LABELS, BAND):
        logits = lax.dot_general(
            rows,
            w_ref[0, c : c + BAND],
            (((1,), (1,)), ((), ())),
            preferred_element_type=jnp.float32,
        )
        place = lax.broadcasted_iota(jnp.int32, logits.shape, 1) + c
        target = jnp.where(tag == place, 1.0, 0.0)
        cols.append((jax.nn.sigmoid(logits) - target).astype(jnp.bfloat16))
    grad = jnp.concatenate(cols, axis=1)
    part = jnp.dot(grad, w_ref[0], preferred_element_type=jnp.float32)
    return grad, part.astype(jnp.bfloat16)


def first_kernel(count, lab_ref, *refs):
    pieces, w_ref, grad_ref, parts = refs[:count], refs[count], refs[count + 1], refs[count + 2 :]
    at = 0
    for k, piece in enumerate(pieces):
        for t in range(0, piece.shape[0], TILE):
            notes = piece[t : t + TILE, D:].astype(jnp.float32)
            grad, part = tile_grads(
                piece[t : t + TILE, :D], notes[:, 0:1], notes[:, 1:2], lab_ref[0] * LABELS, w_ref
            )
            grad_ref[at : at + TILE] = grad
            if len(parts) == 1:
                parts[0][at : at + TILE] = part
            else:
                parts[k][t : t + TILE] = part
            at += TILE


def whole(shape):
    return pl.BlockSpec(shape, lambda *_: (0,) * len(shape))


def first_grads(lab, pieces, weights, apart=False):
    bf = jnp.bfloat16
    n = sum(p.shape[0] for p in pieces)
    sizes = [p.shape[0] for p in pieces] if apart else [n]
    count = len(pieces)
    return pl.pallas_call(
        lambda *refs: first_kernel(count, *refs),
        grid=(1,),
        in_specs=[pl.BlockSpec(memory_space=pltpu.SMEM)]
        + [whole(p.shape) for p in pieces]
        + [whole((1, LABELS, D))],
        out_specs=[whole((n, LABELS))] + [whole((m, D)) for m in sizes],
        out_shape=[jax.ShapeDtypeStruct((n, LABELS), bf)]
        + [jax.ShapeDtypeStruct((m, D), bf) for m in sizes],
        cost_estimate=pl.CostEstimate(
            flops=4 * n * LABELS * D, bytes_accessed=2 * n * 3000, transcendentals=n * LABELS
        ),
        name="first_grads",
    )(lab, *pieces, weights)


def second_kernel(near, lab_ref, rows_ref, *refs):
    count = 5 if near else 2
    notes_refs, w_ref, grad_ref, parts = refs[:count], refs[count], refs[count + 1], refs[count + 2 :]
    block, early = pl.program_id(0), pl.program_id(1) == 0
    notes = [ref[...].astype(jnp.float32) for ref in notes_refs]
    pair = lambda k: jnp.where(early, notes[k], notes[k + 1])
    if near:
        notes = jnp.where(block == 0, notes[0], jnp.where(block == 1, pair(1), pair(3)))
    else:
        notes = pair(0)
    rows = rows_ref[...].reshape(TILE, D)
    grad, part = tile_grads(rows, notes[:, 2:3], notes[:, 3:4], lab_ref[0] * LABELS, w_ref)
    grad_ref[...] = grad
    if near:
        parts[0][0] = part
        return

    @pl.when(early)
    def _():
        parts[0][...] = part

    @pl.when(jnp.logical_not(early))
    def _():
        parts[1][...] = part


def second_grads(lab, rows, blocks, weights, near):
    bf = jnp.bfloat16
    pieces = [p for block in blocks for p in block]
    first, count = (0, LAB - 1) if near else (LAB - 1, 1)
    n = count * ROWS
    source = TILE // CAP
    still = pl.BlockSpec((TILE, TAGS), lambda k, i: (0, D // TAGS))
    each = pl.BlockSpec((TILE, TAGS), lambda k, i: (i, D // TAGS))
    if near:
        part_specs = [pl.BlockSpec((1, TILE, D), lambda k, i: (k, i, 0))]
        part_shapes = [jax.ShapeDtypeStruct((count, ROWS, D), bf)]
    else:
        part_specs = [whole((TILE, D))] * 2
        part_shapes = [jax.ShapeDtypeStruct((TILE, D), bf)] * 2
    return pl.pallas_call(
        lambda *refs: second_kernel(near, *refs),
        grid=(count, 2),
        in_specs=[
            pl.BlockSpec(memory_space=pltpu.SMEM),
            pl.BlockSpec((source, CAP, D), lambda k, i: (i, first + k, 0)),
        ]
        + ([each] if near else [])
        + [still] * (4 if near else 2)
        + [pl.BlockSpec((1, LABELS, D), lambda k, i: (1, 0, 0))],
        out_specs=[pl.BlockSpec((TILE, LABELS), lambda k, i: (2 * k + i, 0))] + part_specs,
        out_shape=[jax.ShapeDtypeStruct((n, LABELS), bf)] + part_shapes,
        cost_estimate=pl.CostEstimate(
            flops=4 * n * LABELS * D, bytes_accessed=2 * n * 3000, transcendentals=n * LABELS
        ),
        name="second_grads",
    )(lab, rows, *pieces, weights)


def update_kernel(counts, *refs):
    grads, rest = refs[: len(counts)], refs[len(counts) :]
    many = max(sum(counts), 1)
    rows, rest = rest[:many], rest[many:]
    w_ref, m_ref, wo_ref, mo_ref = rest[0], rest[1], rest[-2], rest[-1]
    terms = []
    if sum(counts):
        k = 0
        for grad_ref, count in zip(grads, counts):
            at = 0
            for rows_ref in rows[k : k + count]:
                size = rows_ref.shape[0]
                terms.append((grad_ref[at : at + size], rows_ref[:, :D]))
                at += size
            k += count
    else:
        k = 0
        for grad_ref in grads:
            for at in range(0, grad_ref.shape[0], ROWS):
                slots = rows[0][:, k * CAP : (k + 1) * CAP].reshape(ROWS, D)
                terms.append((grad_ref[at : at + ROWS], slots))
                k += 1
    fresh = momentum_decay * m_ref[0]
    for grad, values in terms:
        fresh = fresh + lax.dot_general(
            grad, values, (((0,), (0,)), ((), ())), preferred_element_type=jnp.float32
        )
    mo_ref[0] = fresh
    wo_ref[0] = (w_ref[0].astype(jnp.float32) - step_rate * fresh).astype(jnp.bfloat16)


def update(cluster, grads, blocks, weights, momentum, before=()):
    bands = LABELS // BAND
    band = pl.BlockSpec((1, BAND, D), lambda b: (cluster, b, 0))
    shared = not isinstance(blocks, tuple)
    counts = (0,) * len(grads) if shared else tuple(len(block) for block in blocks)
    rows = [blocks] if shared else [piece for block in blocks for piece in block]
    first = len(grads) + len(rows) + 2
    return pl.pallas_call(
        lambda *refs: update_kernel(counts, *refs),
        grid=(bands,),
        in_specs=[pl.BlockSpec((g.shape[0], BAND), lambda b: (0, b)) for g in grads]
        + [whole(r.shape) for r in rows]
        + [band, band]
        + [pl.BlockSpec(memory_space=pl.ANY) for _ in before],
        out_specs=(band, band),
        out_shape=(
            jax.ShapeDtypeStruct(weights.shape, weights.dtype),
            jax.ShapeDtypeStruct(momentum.shape, momentum.dtype),
        ),
        input_output_aliases={first + k: k for k in range(len(before))},
        cost_estimate=pl.CostEstimate(
            flops=2 * LAB * ROWS * LABELS * D, bytes_accessed=18 << 20, transcendentals=0
        ),
        name="update",
    )(*grads, *rows, weights, momentum, *before)


def swap(x):
    return lax.all_to_all(x, "clus", split_axis=0, concat_axis=0, tiled=True)


def add(*terms):
    total = terms[0].astype(jnp.float32)
    for term in terms[1:]:
        total = total + term.astype(jnp.float32)
    return total.astype(jnp.bfloat16)


def ring_sum(parts):
    own, low, high, far_a, far_b = parts
    half = ROWS // 2
    up = lax.ppermute(far_a, "lab", ring(1))
    down = lax.ppermute(far_b, "lab", ring(-1))
    up = jnp.concatenate([add(high[:half], up), high[half:]])
    down = jnp.concatenate([low[:half], add(low[half:], down)])
    up = lax.ppermute(up, "lab", ring(1))
    down = lax.ppermute(down, "lab", ring(-1))
    return add(own, up, down)


def step(queries, visits, positives, weights, momentum):
    vt, pt = visits.T, positives.T
    bf = jnp.bfloat16
    lab = lax.axis_index("lab").reshape(1).astype(jnp.int32)

    box_a, raw = pl.pallas_call(
        own_kernel,
        out_shape=(
            jax.ShapeDtypeStruct((ROWS, D + TAGS), bf),
            jax.ShapeDtypeStruct((NQ + EXTRA, D), bf),
        ),
        name="own_box",
    )(vt, pt, queries)
    peers = [raw] + [lax.ppermute(raw, "lab", ring(s)) for s in (1, -1, 2)]
    got_a = swap(box_a.reshape(CLUS, CAP, D + TAGS)).reshape(ROWS, D + TAGS)
    box_b = pl.pallas_call(
        all_kernel,
        out_shape=jax.ShapeDtypeStruct((CLUS, LAB, CAP, D), bf),
        name="all_box",
    )(*peers)
    got_b = swap(box_b.reshape(CLUS, LAB * CAP, D))

    half = ROWS // 2
    low_a = lax.ppermute(got_a[:half], "lab", ring(1))
    high_b = lax.ppermute(got_a[half:], "lab", ring(-1))
    low_b = lax.ppermute(got_a[half:], "lab", ring(1))
    high_a = lax.ppermute(got_a[:half], "lab", ring(-1))
    far_a = lax.ppermute(low_a, "lab", ring(1))
    far_b = lax.ppermute(high_b, "lab", ring(-1))
    blocks = ((got_a,), (low_a, low_b), (high_a, high_b), (far_a, far_b))
    grads_a, parts_a = [], []
    for block, place in zip(blocks, ("here", "near1", "near2", "far")):
        grad, *parts = first_grads(lab, block, weights, apart=place == "far")
        grads_a.append(grad)
        parts_a += parts
    home_a = ring_sum(parts_a)
    grad_far, *far_b_parts = second_grads(lab, got_b, blocks[3:], weights, near=False)
    grad_near, parts_near = second_grads(lab, got_b, blocks[:3], weights, near=True)
    home_b = ring_sum([parts_near[0], parts_near[1], parts_near[2]] + far_b_parts)
    home_a = swap(home_a.reshape(CLUS, CAP, D)).reshape(ROWS, D)
    home_b = swap(home_b.reshape(CLUS, CAP, D)).reshape(ROWS, D)
    new = update(0, grads_a, blocks, weights, momentum)
    new = update(1, (grad_near, grad_far), got_b, weights, momentum, new)
    total = ()
    for parity, homed in enumerate((home_a, home_b)):
        query_grad = pl.pallas_call(
            lambda *refs, parity=parity: home_kernel(parity, *refs),
            out_shape=jax.ShapeDtypeStruct((NQ, D), jnp.float32),
            name="home_sum",
        )(vt, homed, *total)
        total = (query_grad,)
    return (query_grad, *new)


def solution(mesh):
    in_specs = (
        P(("clus", "lab"), None),
        P(("clus", "lab"), None),
        P(("clus", "lab"), None),
        P("clus", "lab", None),
        P("clus", "lab", None),
    )
    out_specs = (P(("clus", "lab"), None), P("clus", "lab", None), P("clus", "lab", None))
    return jax.shard_map(step, mesh=mesh, in_specs=in_specs, out_specs=out_specs, check_vma=False)
```

```python
import jax
import jax.numpy as jnp
from jax import lax
from jax.experimental import pallas as pl
from jax.experimental.pallas import tpu as pltpu
from jax.sharding import PartitionSpec as P


momentum_decay = 0.9
step_rate = 0.002

CLUS = 32
LAB = 4
CAP = 16
NQ = 128
VISITS = 4
D = 768
EXTRA = 8
TAGS = 128
TILE = 256
LABELS = 1024
BAND = 256
ROWS = CLUS * CAP


def ring(shift):
    return [(i, (i + shift) % LAB) for i in range(LAB)]


def picks(visits_t, parity):
    dest = lax.broadcasted_iota(jnp.int32, (CLUS, NQ), 0) * 2 + parity
    hit = visits_t[0:1, :] == dest
    for k in range(1, VISITS):
        hit = hit | (visits_t[k : k + 1, :] == dest)
    before = lax.broadcasted_iota(jnp.int32, (NQ, NQ), 0) < lax.broadcasted_iota(
        jnp.int32, (NQ, NQ), 1
    )
    rank = jnp.dot(
        hit.astype(jnp.float32).astype(jnp.bfloat16),
        before.astype(jnp.float32).astype(jnp.bfloat16),
        preferred_element_type=jnp.float32,
    )
    place = jnp.where(hit, rank, -1.0).astype(jnp.int32)
    slot = lax.broadcasted_iota(jnp.int32, (CLUS, CAP, NQ), 1)
    return (place[:, None, :] == slot).reshape(ROWS, NQ)


def as_bf16(flags):
    return flags.astype(jnp.float32).astype(jnp.bfloat16)


def labels_of(visits_t, positives_t, parity):
    dest = lax.broadcasted_iota(jnp.int32, (CLUS, NQ), 0) * 2 + parity
    label = jnp.zeros((CLUS, NQ), jnp.int32)
    for k in range(VISITS):
        label = label + jnp.where(visits_t[k : k + 1, :] == dest, positives_t[k : k + 1, :] + 1, 0)
    return label


def slot_labels(chosen, label):
    wide = jnp.broadcast_to(label[:, None, :], (CLUS, CAP, NQ)).reshape(ROWS, NQ)
    return jnp.sum(jnp.where(chosen, wide, 0), axis=1, keepdims=True) - 1


def own_kernel(visits_ref, positives_ref, queries_ref, box_ref, raw_ref):
    bf = jnp.bfloat16
    visits_t, positives_t = visits_ref[...], positives_ref[...]
    lane = lax.broadcasted_iota(jnp.int32, (ROWS, TAGS), 1)
    notes = jnp.zeros((ROWS, TAGS), jnp.float32)
    for parity in range(2):
        chosen = picks(visits_t, parity)
        label = slot_labels(chosen, labels_of(visits_t, positives_t, parity))
        high = label >> 6
        low = label & 63
        notes = jnp.where(lane == 2 * parity, high.astype(jnp.float32), notes)
        notes = jnp.where(lane == 2 * parity + 1, low.astype(jnp.float32), notes)
        if parity == 0:
            filled = jnp.dot(as_bf16(chosen), queries_ref[...], preferred_element_type=jnp.float32)
            box_ref[:, :D] = filled.astype(bf)
    box_ref[:, D:] = notes.astype(bf)
    raw_ref[:NQ] = queries_ref[...]
    values = visits_t.astype(jnp.float32)
    parts = [values[k : k + 1, :] for k in range(VISITS)]
    row = jnp.concatenate(parts + [jnp.zeros((1, D - VISITS * NQ), jnp.float32)], axis=1)
    raw_ref[NQ:] = jnp.concatenate([row, jnp.zeros((EXTRA - 1, D), jnp.float32)], axis=0).astype(bf)


def all_kernel(*refs):
    box_ref = refs[LAB]
    for k in range(LAB):
        extra = refs[k][NQ:].astype(jnp.float32)
        parts = [extra[0:1, j * NQ : (j + 1) * NQ] for j in range(VISITS)]
        visits_t = jnp.concatenate(parts, axis=0).astype(jnp.int32)
        filled = jnp.dot(
            as_bf16(picks(visits_t, 1)), refs[k][:NQ], preferred_element_type=jnp.float32
        )
        box_ref[:, k] = filled.astype(jnp.bfloat16).reshape(CLUS, CAP, D)


def home_kernel(parity, visits_ref, homed_ref, *refs):
    chosen = as_bf16(picks(visits_ref[...], parity))
    total = lax.dot_general(
        chosen, homed_ref[...], (((0,), (0,)), ((), ())), preferred_element_type=jnp.float32
    )
    for before_ref in refs[:-1]:
        total = total + before_ref[...]
    refs[-1][...] = total


def tile_grads(rows, high, low, first, w_ref):
    tag = (high * 64.0 + low).astype(jnp.int32) - first
    cols = []
    for c in range(0, LABELS, BAND):
        logits = lax.dot_general(
            rows,
            w_ref[0, c : c + BAND],
            (((1,), (1,)), ((), ())),
            preferred_element_type=jnp.float32,
        )
        place = lax.broadcasted_iota(jnp.int32, logits.shape, 1) + c
        target = jnp.where(tag == place, 1.0, 0.0)
        cols.append((jax.nn.sigmoid(logits) - target).astype(jnp.bfloat16))
    grad = jnp.concatenate(cols, axis=1)
    part = jnp.dot(grad, w_ref[0], preferred_element_type=jnp.float32)
    return grad, part.astype(jnp.bfloat16)


def first_kernel(count, lab_ref, *refs):
    pieces, w_ref, grad_ref, parts = refs[:count], refs[count], refs[count + 1], refs[count + 2 :]
    at = 0
    for k, piece in enumerate(pieces):
        for t in range(0, piece.shape[0], TILE):
            notes = piece[t : t + TILE, D:].astype(jnp.float32)
            grad, part = tile_grads(
                piece[t : t + TILE, :D], notes[:, 0:1], notes[:, 1:2], lab_ref[0] * LABELS, w_ref
            )
            grad_ref[at : at + TILE] = grad
            if len(parts) == 1:
                parts[0][at : at + TILE] = part
            else:
                parts[k][t : t + TILE] = part
            at += TILE


def whole(shape):
    return pl.BlockSpec(shape, lambda *_: (0,) * len(shape))


def first_grads(lab, pieces, weights, apart=False):
    bf = jnp.bfloat16
    n = sum(p.shape[0] for p in pieces)
    sizes = [p.shape[0] for p in pieces] if apart else [n]
    count = len(pieces)
    return pl.pallas_call(
        lambda *refs: first_kernel(count, *refs),
        grid=(1,),
        in_specs=[pl.BlockSpec(memory_space=pltpu.SMEM)]
        + [whole(p.shape) for p in pieces]
        + [whole((1, LABELS, D))],
        out_specs=[whole((n, LABELS))] + [whole((m, D)) for m in sizes],
        out_shape=[jax.ShapeDtypeStruct((n, LABELS), bf)]
        + [jax.ShapeDtypeStruct((m, D), bf) for m in sizes],
        cost_estimate=pl.CostEstimate(
            flops=4 * n * LABELS * D, bytes_accessed=2 * n * 3000, transcendentals=n * LABELS
        ),
        name="first_grads",
    )(lab, *pieces, weights)


def second_kernel(near, lab_ref, rows_ref, *refs):
    count = 5 if near else 2
    notes_refs, w_ref, grad_ref, parts = refs[:count], refs[count], refs[count + 1], refs[count + 2 :]
    block, early = pl.program_id(0), pl.program_id(1) == 0
    notes = [ref[...].astype(jnp.float32) for ref in notes_refs]
    pair = lambda k: jnp.where(early, notes[k], notes[k + 1])
    if near:
        notes = jnp.where(block == 0, notes[0], jnp.where(block == 1, pair(1), pair(3)))
    else:
        notes = pair(0)
    rows = rows_ref[...].reshape(TILE, D)
    grad, part = tile_grads(rows, notes[:, 2:3], notes[:, 3:4], lab_ref[0] * LABELS, w_ref)
    grad_ref[...] = grad
    if near:
        parts[0][0] = part
        return

    @pl.when(early)
    def _():
        parts[0][...] = part

    @pl.when(jnp.logical_not(early))
    def _():
        parts[1][...] = part


def second_grads(lab, rows, blocks, weights, near):
    bf = jnp.bfloat16
    pieces = [p for block in blocks for p in block]
    first, count = (0, LAB - 1) if near else (LAB - 1, 1)
    n = count * ROWS
    source = TILE // CAP
    still = pl.BlockSpec((TILE, TAGS), lambda k, i: (0, D // TAGS))
    each = pl.BlockSpec((TILE, TAGS), lambda k, i: (i, D // TAGS))
    if near:
        part_specs = [pl.BlockSpec((1, TILE, D), lambda k, i: (k, i, 0))]
        part_shapes = [jax.ShapeDtypeStruct((count, ROWS, D), bf)]
    else:
        part_specs = [whole((TILE, D))] * 2
        part_shapes = [jax.ShapeDtypeStruct((TILE, D), bf)] * 2
    return pl.pallas_call(
        lambda *refs: second_kernel(near, *refs),
        grid=(count, 2),
        in_specs=[
            pl.BlockSpec(memory_space=pltpu.SMEM),
            pl.BlockSpec((source, CAP, D), lambda k, i: (i, first + k, 0)),
        ]
        + ([each] if near else [])
        + [still] * (4 if near else 2)
        + [pl.BlockSpec((1, LABELS, D), lambda k, i: (1, 0, 0))],
        out_specs=[pl.BlockSpec((TILE, LABELS), lambda k, i: (2 * k + i, 0))] + part_specs,
        out_shape=[jax.ShapeDtypeStruct((n, LABELS), bf)] + part_shapes,
        cost_estimate=pl.CostEstimate(
            flops=4 * n * LABELS * D, bytes_accessed=2 * n * 3000, transcendentals=n * LABELS
        ),
        name="second_grads",
    )(lab, rows, *pieces, weights)


def update_kernel(counts, *refs):
    grads, rest = refs[: len(counts)], refs[len(counts) :]
    many = max(sum(counts), 1)
    rows, rest = rest[:many], rest[many:]
    w_ref, m_ref, wo_ref, mo_ref = rest[0], rest[1], rest[-2], rest[-1]
    terms = []
    if sum(counts):
        k = 0
        for grad_ref, count in zip(grads, counts):
            at = 0
            for rows_ref in rows[k : k + count]:
                size = rows_ref.shape[0]
                terms.append((grad_ref[at : at + size], rows_ref[:, :D]))
                at += size
            k += count
    else:
        k = 0
        for grad_ref in grads:
            for at in range(0, grad_ref.shape[0], ROWS):
                slots = rows[0][:, k * CAP : (k + 1) * CAP].reshape(ROWS, D)
                terms.append((grad_ref[at : at + ROWS], slots))
                k += 1
    fresh = momentum_decay * m_ref[0]
    for grad, values in terms:
        fresh = fresh + lax.dot_general(
            grad, values, (((0,), (0,)), ((), ())), preferred_element_type=jnp.float32
        )
    mo_ref[0] = fresh
    wo_ref[0] = (w_ref[0].astype(jnp.float32) - step_rate * fresh).astype(jnp.bfloat16)


def update(cluster, grads, blocks, weights, momentum, before=()):
    bands = LABELS // BAND
    band = pl.BlockSpec((1, BAND, D), lambda b: (cluster, b, 0))
    shared = not isinstance(blocks, tuple)
    counts = (0,) * len(grads) if shared else tuple(len(block) for block in blocks)
    rows = [blocks] if shared else [piece for block in blocks for piece in block]
    first = len(grads) + len(rows) + 2
    return pl.pallas_call(
        lambda *refs: update_kernel(counts, *refs),
        grid=(bands,),
        in_specs=[pl.BlockSpec((g.shape[0], BAND), lambda b: (0, b)) for g in grads]
        + [whole(r.shape) for r in rows]
        + [band, band]
        + [pl.BlockSpec(memory_space=pl.ANY) for _ in before],
        out_specs=(band, band),
        out_shape=(
            jax.ShapeDtypeStruct(weights.shape, weights.dtype),
            jax.ShapeDtypeStruct(momentum.shape, momentum.dtype),
        ),
        input_output_aliases={first + k: k for k in range(len(before))},
        cost_estimate=pl.CostEstimate(
            flops=2 * LAB * ROWS * LABELS * D, bytes_accessed=18 << 20, transcendentals=0
        ),
        name="update",
    )(*grads, *rows, weights, momentum, *before)


def swap(x):
    return lax.all_to_all(x, "clus", split_axis=0, concat_axis=0, tiled=True)


def add(*terms):
    total = terms[0].astype(jnp.float32)
    for term in terms[1:]:
        total = total + term.astype(jnp.float32)
    return total.astype(jnp.bfloat16)


def early_ring_sum(parts):
    own, low, high, far_a, far_b = parts
    half = ROWS // 2
    up = lax.ppermute(far_a, "lab", ring(1))
    down = lax.ppermute(far_b, "lab", ring(-1))
    up_rest = lax.ppermute(high[half:], "lab", ring(1))
    down_rest = lax.ppermute(low[:half], "lab", ring(-1))
    up, down = add(high[:half], up), add(low[half:], down)
    up = lax.ppermute(up, "lab", ring(1))
    down = lax.ppermute(down, "lab", ring(-1))
    return jnp.concatenate([add(own[:half], up, down_rest), add(own[half:], up_rest, down)])


def ring_sum(parts):
    own, low, high, far_a, far_b = parts
    half = ROWS // 2
    up = lax.ppermute(far_a, "lab", ring(1))
    down = lax.ppermute(far_b, "lab", ring(-1))
    up = jnp.concatenate([add(high[:half], up), high[half:]])
    down = jnp.concatenate([low[:half], add(low[half:], down)])
    up = lax.ppermute(up, "lab", ring(1))
    down = lax.ppermute(down, "lab", ring(-1))
    return add(own, up, down)


def step(queries, visits, positives, weights, momentum):
    vt, pt = visits.T, positives.T
    bf = jnp.bfloat16
    lab = lax.axis_index("lab").reshape(1).astype(jnp.int32)

    box_a, raw = pl.pallas_call(
        own_kernel,
        out_shape=(
            jax.ShapeDtypeStruct((ROWS, D + TAGS), bf),
            jax.ShapeDtypeStruct((NQ + EXTRA, D), bf),
        ),
        name="own_box",
    )(vt, pt, queries)
    peers = [raw] + [lax.ppermute(raw, "lab", ring(s)) for s in (1, -1, 2)]
    got_a = swap(box_a.reshape(CLUS, CAP, D + TAGS)).reshape(ROWS, D + TAGS)
    box_b = pl.pallas_call(
        all_kernel,
        out_shape=jax.ShapeDtypeStruct((CLUS, LAB, CAP, D), bf),
        name="all_box",
    )(*peers)
    got_b = swap(box_b.reshape(CLUS, LAB * CAP, D))

    half = ROWS // 2
    low_a = lax.ppermute(got_a[:half], "lab", ring(1))
    high_b = lax.ppermute(got_a[half:], "lab", ring(-1))
    low_b = lax.ppermute(got_a[half:], "lab", ring(1))
    high_a = lax.ppermute(got_a[:half], "lab", ring(-1))
    far_a = lax.ppermute(low_a, "lab", ring(1))
    far_b = lax.ppermute(high_b, "lab", ring(-1))
    blocks = ((got_a,), (low_a, low_b), (high_a, high_b), (far_a, far_b))
    grads_a, parts_a = [], []
    for block, place in zip(blocks, ("here", "near1", "near2", "far")):
        grad, *parts = first_grads(lab, block, weights, apart=place == "far")
        grads_a.append(grad)
        parts_a += parts
    home_a = early_ring_sum(parts_a)
    grad_far, *far_b_parts = second_grads(lab, got_b, blocks[3:], weights, near=False)
    grad_near, parts_near = second_grads(lab, got_b, blocks[:3], weights, near=True)
    home_b = ring_sum([parts_near[0], parts_near[1], parts_near[2]] + far_b_parts)
    home_a = swap(home_a.reshape(CLUS, CAP, D)).reshape(ROWS, D)
    home_b = swap(home_b.reshape(CLUS, CAP, D)).reshape(ROWS, D)
    new = update(0, grads_a, blocks, weights, momentum)
    new = update(1, (grad_near, grad_far), got_b, weights, momentum, new)
    total = ()
    for parity, homed in enumerate((home_a, home_b)):
        query_grad = pl.pallas_call(
            lambda *refs, parity=parity: home_kernel(parity, *refs),
            out_shape=jax.ShapeDtypeStruct((NQ, D), jnp.float32),
            name="home_sum",
        )(vt, homed, *total)
        total = (query_grad,)
    return (query_grad, *new)


def solution(mesh):
    in_specs = (
        P(("clus", "lab"), None),
        P(("clus", "lab"), None),
        P(("clus", "lab"), None),
        P("clus", "lab", None),
        P("clus", "lab", None),
    )
    out_specs = (P(("clus", "lab"), None), P("clus", "lab", None), P("clus", "lab", None))
    return jax.shard_map(step, mesh=mesh, in_specs=in_specs, out_specs=out_specs, check_vma=False)
```
